128 devices in a mesh: dp: 1, tp: 2 (over core), cp: 64 (over z, y, x).
Axes of the slice: x: 4, y: 4, z: 4, core: 2. Of those that a mesh axis runs over, the one named last changes fastest.
Arguments:
- hidden_in: bfloat16 [8192, 1536], P(('dp', 'cp', 'tp'))
- positions: int32 [8192], P(('dp', 'cp', 'tp'))
- cache_len: int32 [1], P('dp')
- cache_k: bfloat16 [32768, 256], P(('dp', 'cp', 'tp'))
- cache_v: bfloat16 [32768, 256], P(('dp', 'cp', 'tp'))
- norm1_gain: bfloat16 [1536], replicated
- w_query: bfloat16 [1536, 1536], P(None, 'tp')
- w_key: bfloat16 [1536, 256], P(None, 'tp')
- w_value: bfloat16 [1536, 256], P(None, 'tp')
- w_out: bfloat16 [1536, 1536], P('tp')
- norm2_gain: bfloat16 [1536], replicated
- w_gate: bfloat16 [1536, 8960], P(None, 'tp')
- w_up: bfloat16 [1536, 8960], P(None, 'tp')
- w_down: bfloat16 [8960, 1536], P('tp')
Outputs:
- output: bfloat16 [8192, 1536], P(('dp', 'cp', 'tp'))
All inputs are finite; a program needn't handle non-finite values.
Results may differ from the reference program's by a relative error of at most 0.011224.
Values are sent between devices in bfloat16 or wider.
A program may use at most 1 GiB of HBM per device.

```python
import math
import jax
import jax.numpy as jnp
from jax import lax

TOKENS = 8192
PREFIX = 32768
D_MODEL = 1536
Q_HEADS = 12
KV_HEADS = 2
HEAD_DIM = 128
FFN_DIM = 8960
SHARD_COUNT = 128
SHARD_ROWS = 64
QUERY_BLOCK = 64
ROPE_BASE = 500000.0
NORM_EPS = 1e-5


def normal_draw(rand_key, out_shape, spread):
    return (jax.random.normal(rand_key, out_shape, jnp.float32) * spread).astype(jnp.bfloat16)


def setup_inputs(seed: int = 0, part: int = 0) -> dict:
    base_key = jax.random.key(seed)
    part_keys = jax.random.split(jax.random.fold_in(base_key, part), 4)
    shared_keys = jax.random.split(jax.random.key(seed + 1), 9)
    cache_len = jax.random.randint(part_keys[0], (1,), PREFIX // 16, PREFIX + 1, dtype=jnp.int32)
    row_ids = jnp.arange(TOKENS, dtype=jnp.int32)
    half_rows = SHARD_ROWS // 2
    shard_ids = row_ids // SHARD_ROWS
    within = row_ids % SHARD_ROWS
    segment = jnp.where(within < half_rows, shard_ids, 2 * SHARD_COUNT - 1 - shard_ids)
    positions = cache_len[0] + segment * half_rows + within % half_rows
    qk_std = math.log((PREFIX + TOKENS) / 4.0) ** 0.25
    width_std = D_MODEL ** -0.5
    kv_width = KV_HEADS * HEAD_DIM
    return {
        'hidden_in': normal_draw(part_keys[1], (TOKENS, D_MODEL), 1.0),
        'positions': positions,
        'cache_len': cache_len,
        'cache_k': normal_draw(part_keys[2], (PREFIX, kv_width), qk_std),
        'cache_v': normal_draw(part_keys[3], (PREFIX, kv_width), 1.0),
        'norm1_gain': (1.0 + 0.3 * jax.random.normal(shared_keys[0], (D_MODEL,), jnp.float32)).astype(jnp.bfloat16),
        'w_query': normal_draw(shared_keys[1], (D_MODEL, Q_HEADS * HEAD_DIM), qk_std * width_std),
        'w_key': normal_draw(shared_keys[2], (D_MODEL, kv_width), qk_std * width_std),
        'w_value': normal_draw(shared_keys[3], (D_MODEL, kv_width), width_std),
        'w_out': normal_draw(shared_keys[4], (Q_HEADS * HEAD_DIM, D_MODEL), 2.0 * (Q_HEADS * HEAD_DIM) ** -0.5),
        'norm2_gain': (1.0 + 0.3 * jax.random.normal(shared_keys[5], (D_MODEL,), jnp.float32)).astype(jnp.bfloat16),
        'w_gate': normal_draw(shared_keys[6], (D_MODEL, FFN_DIM), width_std),
        'w_up': normal_draw(shared_keys[7], (D_MODEL, FFN_DIM), width_std),
        'w_down': normal_draw(shared_keys[8], (FFN_DIM, D_MODEL), FFN_DIM ** -0.5),
    }


def rms_norm(hidden, norm_gain):
    values = hidden.astype(jnp.float32)
    inv_rms = lax.rsqrt(jnp.mean(values * values, axis=-1, keepdims=True) + NORM_EPS)
    return (values * inv_rms * norm_gain.astype(jnp.float32)).astype(jnp.bfloat16)


def rotary(projected, positions):
    half_dim = HEAD_DIM // 2
    inv_freq = 1.0 / (ROPE_BASE ** (jnp.arange(half_dim, dtype=jnp.float32) * (2.0 / HEAD_DIM)))
    angles = positions.astype(jnp.float32)[:, None] * inv_freq[None, :]
    expand = (angles.shape[0],) + (1,) * (projected.ndim - 2) + (half_dim,)
    cos_table = jnp.cos(angles).reshape(expand)
    sin_table = jnp.sin(angles).reshape(expand)
    first_half = projected[..., :half_dim]
    second_half = projected[..., half_dim:]
    rotated = jnp.concatenate([first_half * cos_table - second_half * sin_table, second_half * cos_table + first_half * sin_table], axis=-1)
    return rotated.astype(jnp.bfloat16)


def reference(hidden_in, positions, cache_len, cache_k, cache_v, norm1_gain, w_query, w_key, w_value, w_out, norm2_gain, w_gate, w_up, w_down):
    groups = Q_HEADS // KV_HEADS
    block_count = TOKENS // QUERY_BLOCK
    score_scale = 1.0 / math.sqrt(HEAD_DIM)
    normed = rms_norm(hidden_in, norm1_gain)
    queries = rotary(jnp.dot(normed, w_query, preferred_element_type=jnp.float32).reshape(TOKENS, KV_HEADS, groups, HEAD_DIM), positions)
    new_keys = rotary(jnp.dot(normed, w_key, preferred_element_type=jnp.float32).reshape(TOKENS, KV_HEADS, HEAD_DIM), positions)
    new_values = jnp.dot(normed, w_value, preferred_element_type=jnp.float32).astype(jnp.bfloat16).reshape(TOKENS, KV_HEADS, HEAD_DIM)
    head_keys = jnp.moveaxis(new_keys, 1, 0)
    head_values = jnp.moveaxis(new_values, 1, 0)
    cached_keys = jnp.moveaxis(cache_k.reshape(PREFIX, KV_HEADS, HEAD_DIM), 1, 0)
    cached_values = jnp.moveaxis(cache_v.reshape(PREFIX, KV_HEADS, HEAD_DIM), 1, 0)
    cache_valid = jnp.arange(PREFIX) < cache_len[0]
    query_blocks = jnp.moveaxis(queries.reshape(block_count, QUERY_BLOCK, KV_HEADS, groups, HEAD_DIM), 2, 1)
    position_blocks = positions.reshape(block_count, QUERY_BLOCK)

    def attend_block(block_item):
        block_queries, block_pos = block_item
        causal = positions[None, None, :] <= block_pos[None, :, None]

        def attend_head(head_item):
            head_queries, cache_key_head, cache_value_head, new_key_head, new_value_head = head_item
            query_wide = head_queries.astype(jnp.float32)
            cache_scores = jnp.einsum('rgd,sd->grs', query_wide, cache_key_head.astype(jnp.float32)) * score_scale
            new_scores = jnp.einsum('rgd,sd->grs', query_wide, new_key_head.astype(jnp.float32)) * score_scale
            cache_scores = jnp.where(cache_valid[None, None, :], cache_scores, -jnp.inf)
            new_scores = jnp.where(causal, new_scores, -jnp.inf)
            row_max = jnp.maximum(jnp.max(cache_scores, axis=-1, keepdims=True), jnp.max(new_scores, axis=-1, keepdims=True))
            cache_probs = jnp.exp(cache_scores - row_max)
            new_probs = jnp.exp(new_scores - row_max)
            normalizer = jnp.sum(cache_probs, axis=-1, keepdims=True) + jnp.sum(new_probs, axis=-1, keepdims=True)
            weighted = jnp.einsum('grs,sd->grd', cache_probs.astype(jnp.bfloat16).astype(jnp.float32), cache_value_head.astype(jnp.float32))
            weighted = weighted + jnp.einsum('grs,sd->grd', new_probs.astype(jnp.bfloat16).astype(jnp.float32), new_value_head.astype(jnp.float32))
            return (weighted / normalizer).astype(jnp.bfloat16)

        return lax.map(attend_head, (block_queries, cached_keys, cached_values, head_keys, head_values))

    attended = lax.map(attend_block, (query_blocks, position_blocks))
    attended = jnp.transpose(attended, (0, 3, 1, 2, 4)).reshape(TOKENS, Q_HEADS * HEAD_DIM)
    residual_mid = (hidden_in.astype(jnp.float32) + jnp.dot(attended, w_out, preferred_element_type=jnp.float32)).astype(jnp.bfloat16)
    normed_mid = rms_norm(residual_mid, norm2_gain)
    gate_proj = jnp.dot(normed_mid, w_gate, preferred_element_type=jnp.float32)
    up_proj = jnp.dot(normed_mid, w_up, preferred_element_type=jnp.float32)
    hidden_mlp = (jax.nn.silu(gate_proj) * up_proj).astype(jnp.bfloat16)
    return (residual_mid.astype(jnp.float32) + jnp.dot(hidden_mlp, w_down, preferred_element_type=jnp.float32)).astype(jnp.bfloat16)
```

```python
import functools
import math
import jax
import jax.numpy as jnp
from jax import lax
from jax.experimental import pallas as pl
from jax.experimental.pallas import tpu as pltpu
from jax.sharding import PartitionSpec as P

HEAD_DIM = 128
ROPE_BASE = 500000.0
NORM_EPS = 1e-5
HEADS = 6
SLOTS = 256
COLS = HEADS * 64
QW = 4 * COLS
NEG = -2.3e38
EXP_C = math.log2(math.e) / math.sqrt(HEAD_DIM)
BUCKETS = (16,)


def rms_norm(hidden, norm_gain):
    values = hidden.astype(jnp.float32)
    inv_rms = lax.rsqrt(jnp.mean(values * values, axis=-1, keepdims=True) + NORM_EPS)
    return (values * inv_rms * norm_gain.astype(jnp.float32)).astype(jnp.bfloat16)


def rotary(projected, positions):
    half_dim = HEAD_DIM // 2
    inv_freq = 1.0 / (ROPE_BASE ** (jnp.arange(half_dim, dtype=jnp.float32) * (2.0 / HEAD_DIM)))
    angles = positions.astype(jnp.float32)[:, None] * inv_freq[None, :]
    expand = (angles.shape[0],) + (1,) * (projected.ndim - 2) + (half_dim,)
    cos_table = jnp.cos(angles).reshape(expand)
    sin_table = jnp.sin(angles).reshape(expand)
    first_half = projected[..., :half_dim]
    second_half = projected[..., half_dim:]
    rotated = jnp.concatenate([first_half * cos_table - second_half * sin_table, second_half * cos_table + first_half * sin_table], axis=-1)
    return rotated.astype(jnp.bfloat16)


def plane_of(cyc, k):
    major = k // 4
    minor = (k - major) % 4
    return (4 * major + minor) * (1 - cyc) + (4 * minor + major) * cyc


def attend_kernel(nb, mask_from, len_ref, qt_ref, kvn_ref, ck_ref, cv_ref, out_ref,
                  QT, KC, VC, KVN, ACC, PART, VTS,
                  send_sem, recv_sem, q_send, q_recv, o_send, o_recv, sib_send, sib_recv, loc_sem):
    c = lax.axis_index('cp')
    t = lax.axis_index('tp')
    z, y, x = c // 16, (c // 4) % 4, c % 4
    g = 4 * z + y
    k_own = (4 * z + (y + z) % 4, 4 * y + (y + z) % 4)
    cache_len = len_ref[0]

    def dev(core, chip):
        return {'tp': core, 'cp': chip}

    def ring_k(cyc):
        return k_own[0] * (1 - cyc) + k_own[1] * cyc

    def neighbour(cyc, d):
        return plane_of(cyc, (ring_k(cyc) + 1 + 14 * d) % 16) * 4 + x

    def block_of(cyc, d, j):
        return plane_of(cyc, (ring_k(cyc) + 16 + (2 * d - 1) * j) % 16)

    barrier = pltpu.get_barrier_semaphore()
    partners = [dev(t, neighbour(cyc, d)) for cyc in (0, 1) for d in (0, 1)]
    partners += [dev(t, g * 4 + (x + dx) % 4) for dx in (1, 2, 3)] + [dev(1 - t, c)]
    VTS[...] = cv_ref[...].T
    for p in partners:
        pl.semaphore_signal(barrier, inc=1, device_id=p, device_id_type=pl.DeviceIdType.MESH)
    pl.semaphore_wait(barrier, len(partners))

    def q_copy(dx):
        return pltpu.make_async_remote_copy(
            src_ref=qt_ref, dst_ref=QT.at[:, :, pl.ds(pl.multiple_of(x * COLS, 128), COLS)],
            send_sem=q_send.at[dx - 1], recv_sem=q_recv.at[dx - 1],
            device_id=dev(t, g * 4 + (x + dx) % 4), device_id_type=pl.DeviceIdType.MESH)

    def q_land(dx):
        src_x = (x + 4 - dx) % 4
        return pltpu.make_async_remote_copy(
            src_ref=qt_ref, dst_ref=QT.at[:, :, pl.ds(pl.multiple_of(src_x * COLS, 128), COLS)],
            send_sem=q_send.at[dx - 1], recv_sem=q_recv.at[dx - 1],
            device_id=dev(t, g * 4 + (x + dx) % 4), device_id_type=pl.DeviceIdType.MESH)

    mine = pl.ds(pl.multiple_of(t * 128, 128), 128)
    other = pl.ds(pl.multiple_of((1 - t) * 128, 128), 128)

    def sib_copies(half):
        return (pltpu.make_async_remote_copy(
                    src_ref=ck_ref.at[:, other], dst_ref=KC.at[half, g], send_sem=sib_send.at[0], recv_sem=sib_recv.at[0],
                    device_id=dev(1 - t, c), device_id_type=pl.DeviceIdType.MESH),
                pltpu.make_async_remote_copy(
                    src_ref=VTS.at[other], dst_ref=VC.at[half, g], send_sem=sib_send.at[1], recv_sem=sib_recv.at[1],
                    device_id=dev(1 - t, c), device_id_type=pl.DeviceIdType.MESH))

    local = [pltpu.make_async_copy(qt_ref, QT.at[:, :, pl.ds(pl.multiple_of(x * COLS, 128), COLS)], loc_sem.at[0]),
             pltpu.make_async_copy(kvn_ref, KVN.at[g], loc_sem.at[1])]
    local_cache = [pltpu.make_async_copy(ck_ref.at[:, mine], KC.at[t, g], loc_sem.at[2]),
                   pltpu.make_async_copy(VTS.at[mine], VC.at[t, g], loc_sem.at[3])]

    @pl.when(g < nb)
    def _():
        for cp in sib_copies(t):
            cp.start()
        for cp in local_cache:
            cp.start()
    for cp in local:
        cp.start()
    for dx in (2, 1, 3):
        q_copy(dx).start()

    def ring_copy(cyc, d, kind, s, place):
        buf = (KC.at[cyc, place], VC.at[cyc, place], KVN.at[place, cyc])[kind]
        return pltpu.make_async_remote_copy(
            src_ref=buf, dst_ref=buf, send_sem=send_sem.at[cyc, d, kind, s], recv_sem=recv_sem.at[cyc, d, kind, s],
            device_id=dev(t, neighbour(cyc, d)), device_id_type=pl.DeviceIdType.MESH)

    def for_copies(s, fn, back):
        for kind in range(3):
            for cyc in (0, 1):
                for d in (0, 1):
                    place = block_of(cyc, d, s - back)
                    live = s <= 8 - d
                    if kind < 2:
                        live = jnp.logical_and(live, place < nb)

                    @pl.when(live)
                    def _():
                        fn(ring_copy(cyc, d, kind, s, place))

    for cp in local:
        cp.wait()

    @pl.when(g < nb)
    def _():
        for cp in local_cache:
            cp.wait()
        for cp in sib_copies(1 - t):
            cp.wait_recv()

    for_copies(1, lambda cp: cp.start(), 1)

    ACC[:, 128:136, :] = jnp.where(lax.broadcasted_iota(jnp.int32, (2, 8, QW), 1) == 0, NEG, 0.0)
    ACC[:, 0:128, :] = jnp.zeros((2, 128, QW), jnp.float32)

    def units(half, tiles, key, val_t, mask):
        cols = [pl.ds(pl.multiple_of(tile * 256, 256), 256) for tile in tiles]
        scores = [jnp.dot(key, QT[half, :, col], preferred_element_type=jnp.float32) for col in cols]
        if mask is not None:
            scores = [mask(tile, s) for tile, s in zip(tiles, scores)]
        for col, s in zip(cols, scores):
            old_max = ACC[half, 128:129, col]
            new_max = jnp.maximum(old_max, jnp.max(s, axis=0, keepdims=True))
            probs = jnp.exp2(s * EXP_C - new_max * EXP_C)
            alpha = jnp.exp2((old_max - new_max) * EXP_C)
            ACC[half, 128:129, col] = new_max
            ACC[half, 129:130, col] = ACC[half, 129:130, col] * alpha + jnp.sum(probs, axis=0, keepdims=True)
            ACC[half, 0:128, col] = ACC[half, 0:128, col] * alpha + jnp.dot(
                val_t, probs.astype(jnp.bfloat16), preferred_element_type=jnp.float32)

    def cache_block(cyc, place):
        limit = cache_len - (4 * place + x) * (2 * SLOTS) - cyc * SLOTS

        def run(mask):
            def body(i, carry):
                half = i // 3
                pair = i % 3
                units(half, (2 * pair, 2 * pair + 1), KC[cyc, place], VC[cyc, place], mask)
                return carry
            lax.fori_loop(0, 6, body, 0)

        def slot_mask(tile, s):
            return jnp.where(lax.broadcasted_iota(jnp.int32, s.shape, 0) < limit, s, NEG)

        if mask_from > 0:
            @pl.when(place < mask_from)
            def _():
                run(None)

        @pl.when(place >= mask_from)
        def _():
            run(slot_mask)

    for dx in (1, 3, 2):
        q_land(dx).wait_recv()

    def step(s, carry):
        for_copies(s, lambda cp: cp.wait_recv(), 0)
        for_copies(s + 1, lambda cp: cp.start(), 1)
        j = s - 1

        def block(b, inner):
            cyc, d = b // 2, b % 2
            place = block_of(cyc, d, j)
            live = jnp.logical_and(place < nb, jnp.logical_or(d == 0, jnp.logical_and(j > 0, j < 8)))

            @pl.when(live)
            def _():
                cache_block(cyc, place)
            return inner
        lax.fori_loop(0, 4, block, 0)
        return carry

    lax.fori_loop(1, 10, step, 0)

    edge = g // 4

    def new_item(n, carry):
        j = n - 4
        masked_hi = jnp.logical_and(n >= 4, j > edge).astype(jnp.int32)
        masked_lo = jnp.logical_and(n >= 4, j <= edge).astype(jnp.int32)
        full = (n < 4).astype(jnp.int32)
        q_half = 1 - masked_lo
        k_half = masked_hi
        blk = full * n + masked_lo * j + masked_hi * (j - 1)
        places = pl.ds(blk * 4, 4)
        key = KVN[places, :, 0, k_half].reshape(256, 128)
        val_t = KVN[places, :, 1, k_half].reshape(256, 128).T

        def causal(tile, s):
            row = lax.broadcasted_iota(jnp.int32, (256, 1), 0)
            run = 2 * (4 * (blk * 4 + row // 64) + x) + (row % 64) // 32
            key_pos = (run + k_half * (255 - 2 * run)) * 32 + row % 32
            col = lax.broadcasted_iota(jnp.int32, (1, 256), 1) + tile * 256
            q_run = 2 * (4 * g + col // COLS) + (col % 64) // 32
            q_pos = (q_run + q_half * (255 - 2 * q_run)) * 32 + col % 32
            return jnp.where(key_pos <= q_pos, s, NEG)

        def body(i, inner):
            units(q_half, (2 * i, 2 * i + 1), key, val_t, causal)
            return inner
        lax.fori_loop(0, 3, body, 0)
        return carry

    lax.fori_loop(0, 9, new_item, 0)

    def o_copy(dx):
        dst_x = (x + dx) % 4
        return pltpu.make_async_remote_copy(
            src_ref=ACC.at[:, :, pl.ds(pl.multiple_of(dst_x * COLS, 128), COLS)], dst_ref=PART.at[dx - 1],
            send_sem=o_send.at[dx - 1], recv_sem=o_recv.at[dx - 1],
            device_id=dev(t, g * 4 + dst_x), device_id_type=pl.DeviceIdType.MESH)

    for dx in (2, 1, 3):
        o_copy(dx).start()
    for dx in (1, 3, 2):
        o_copy(dx).wait_recv()
    own = pl.ds(pl.multiple_of(x * COLS, 128), COLS)
    for half in (0, 1):
        maxes = [ACC[half, 128:129, own]] + [PART[i, half, 128:129, :] for i in range(3)]
        sums = [ACC[half, 129:130, own]] + [PART[i, half, 129:130, :] for i in range(3)]
        top = functools.reduce(jnp.maximum, maxes)
        weights = [jnp.exp2((m - top) * EXP_C) for m in maxes]
        total = sum(w * l for w, l in zip(weights, sums))
        acc = ACC[half, 0:128, own] * weights[0]
        for i in range(3):
            acc = acc + PART[i, half, 0:128, :] * weights[i + 1]
        o_rows = (acc / total).T.astype(jnp.bfloat16)
        for head in range(HEADS):
            for core in (0, 1):
                out_ref[core * 64 + half * 32:core * 64 + half * 32 + 32, head * 128:head * 128 + 128] = \
                    o_rows[head * 64 + core * 32:head * 64 + core * 32 + 32, :]

    for dx in (1, 2, 3):
        q_copy(dx).wait_send()
        o_copy(dx).wait_send()

    @pl.when(g < nb)
    def _():
        for cp in sib_copies(t):
            cp.wait_send()

    def drain(s, carry):
        for_copies(s, lambda cp: cp.wait_send(), 1)
        return carry
    lax.fori_loop(1, 9, drain, 0)


def attend(index, nb, mask_from, cache_len, q_t, kv_new, cache_k, cache_v):
    bf16, f32 = jnp.bfloat16, jnp.float32
    vmem = pl.BlockSpec(memory_space=pltpu.VMEM)
    return pl.pallas_call(
        functools.partial(attend_kernel, nb, mask_from),
        out_shape=jax.ShapeDtypeStruct((128, HEADS * HEAD_DIM), bf16),
        in_specs=[pl.BlockSpec(memory_space=pltpu.SMEM), vmem, vmem, vmem, vmem],
        out_specs=vmem,
        scratch_shapes=[
            pltpu.VMEM((2, 128, QW), bf16),
            pltpu.VMEM((2, 16, SLOTS, 128), bf16),
            pltpu.VMEM((2, 16, 128, SLOTS), bf16),
            pltpu.VMEM((16, 2, 2, 2, 32, 128), bf16),
            pltpu.VMEM((2, 136, QW), f32),
            pltpu.VMEM((3, 2, 136, COLS), f32),
            pltpu.VMEM((256, SLOTS), bf16),
            pltpu.SemaphoreType.DMA((2, 2, 3, 9)),
            pltpu.SemaphoreType.DMA((2, 2, 3, 9)),
            pltpu.SemaphoreType.DMA((3,)),
            pltpu.SemaphoreType.DMA((3,)),
            pltpu.SemaphoreType.DMA((3,)),
            pltpu.SemaphoreType.DMA((3,)),
            pltpu.SemaphoreType.DMA((2,)),
            pltpu.SemaphoreType.DMA((2,)),
            pltpu.SemaphoreType.DMA((4,)),
        ],
        compiler_params=pltpu.CompilerParams(collective_id=index, has_side_effects=True, vmem_limit_bytes=48 * 1024 * 1024),
        name='attend_%d' % nb,
    )(cache_len, q_t, kv_new, cache_k, cache_v)


def solution(mesh):
    token_spec = P(('dp', 'cp', 'tp'), None)
    column_spec = P(None, 'tp')
    row_spec = P('tp', None)

    def device_layer(hidden_loc, pos_loc, cache_len, cache_k, cache_v, norm1_gain, w_query, w_key, w_value, w_out, norm2_gain, w_gate, w_up, w_down):
        normed = rms_norm(hidden_loc, norm1_gain)
        group_in = lax.all_gather(normed, 'tp', axis=0, tiled=True)
        group_pos = lax.all_gather(pos_loc, 'tp', axis=0, tiled=True)
        rows = group_in.shape[0]
        queries = rotary(jnp.dot(group_in, w_query, preferred_element_type=jnp.float32).reshape(rows, HEADS, HEAD_DIM), group_pos)
        keys_new = rotary(jnp.dot(group_in, w_key, preferred_element_type=jnp.float32), group_pos)
        values_new = jnp.dot(group_in, w_value, preferred_element_type=jnp.float32).astype(jnp.bfloat16)
        q_t = jnp.transpose(queries.reshape(2, 2, 32, HEADS, HEAD_DIM), (1, 4, 3, 0, 2)).reshape(2, HEAD_DIM, COLS)
        kv_new = jnp.stack([keys_new.reshape(2, 2, 32, HEAD_DIM), values_new.reshape(2, 2, 32, HEAD_DIM)], axis=1)
        attended = attend(0, 16, 0, cache_len, q_t, kv_new, cache_k, cache_v)
        attn_part = jnp.dot(attended, w_out, preferred_element_type=jnp.float32)
        residual_mid = (hidden_loc.astype(jnp.float32) + lax.psum_scatter(attn_part, 'tp', scatter_dimension=0, tiled=True)).astype(jnp.bfloat16)
        group_mid = lax.all_gather(rms_norm(residual_mid, norm2_gain), 'tp', axis=0, tiled=True)
        gate_proj = jnp.dot(group_mid, w_gate, preferred_element_type=jnp.float32)
        up_proj = jnp.dot(group_mid, w_up, preferred_element_type=jnp.float32)
        hidden_mlp = (jax.nn.silu(gate_proj) * up_proj).astype(jnp.bfloat16)
        mlp_part = jnp.dot(hidden_mlp, w_down, preferred_element_type=jnp.float32)
        return (residual_mid.astype(jnp.float32) + lax.psum_scatter(mlp_part, 'tp', scatter_dimension=0, tiled=True)).astype(jnp.bfloat16)

    return jax.shard_map(device_layer, mesh=mesh, in_specs=(token_spec, P(('dp', 'cp', 'tp')), P('dp'), token_spec, token_spec, P(), column_spec, column_spec, column_spec, row_spec, P(), column_spec, column_spec, row_spec), out_specs=token_spec, check_vma=False)
```

```python
import functools
import math
import jax
import jax.numpy as jnp
from jax import lax
from jax.experimental import pallas as pl
from jax.experimental.pallas import tpu as pltpu
from jax.sharding import PartitionSpec as P

HEAD_DIM = 128
ROPE_BASE = 500000.0
NORM_EPS = 1e-5
HEADS = 6
SLOTS = 256
COLS = HEADS * 64
QW = 4 * COLS
NEG = -2.3e38
EXP_C = math.log2(math.e) / math.sqrt(HEAD_DIM)
BUCKETS = 8


def rms_norm(hidden, norm_gain):
    values = hidden.astype(jnp.float32)
    inv_rms = lax.rsqrt(jnp.mean(values * values, axis=-1, keepdims=True) + NORM_EPS)
    return (values * inv_rms * norm_gain.astype(jnp.float32)).astype(jnp.bfloat16)


def rotary(projected, positions):
    half_dim = HEAD_DIM // 2
    inv_freq = 1.0 / (ROPE_BASE ** (jnp.arange(half_dim, dtype=jnp.float32) * (2.0 / HEAD_DIM)))
    angles = positions.astype(jnp.float32)[:, None] * inv_freq[None, :]
    expand = (angles.shape[0],) + (1,) * (projected.ndim - 2) + (half_dim,)
    cos_table = jnp.cos(angles).reshape(expand)
    sin_table = jnp.sin(angles).reshape(expand)
    first_half = projected[..., :half_dim]
    second_half = projected[..., half_dim:]
    rotated = jnp.concatenate([first_half * cos_table - second_half * sin_table, second_half * cos_table + first_half * sin_table], axis=-1)
    return rotated.astype(jnp.bfloat16)


def plane_of(cyc, k):
    major = k // 4
    minor = (k - major) % 4
    return (4 * major + minor) * (1 - cyc) + (4 * minor + major) * cyc


def attend_kernel(nb, len_ref, qt_ref, kvn_ref, ck_ref, cv_ref, out_ref,
                  QT, KC, VC, KVN, ACC, PART, VTS,
                  send_sem, recv_sem, q_send, q_recv, o_send, o_recv, sib_send, sib_recv, loc_sem):
    c = lax.axis_index('cp')
    t = lax.axis_index('tp')
    x = c % 4
    g = c // 4
    cache_len = len_ref[0]
    plain_nb = nb - 2

    def dev(core, chip):
        return {'tp': core, 'cp': chip}

    def ring_k(place, cyc):
        zz, yy = place // 4, place % 4
        return (4 * zz) * (1 - cyc) + (4 * yy) * cyc + (yy + zz) % 4

    def neighbour(cyc, d):
        return plane_of(cyc, (ring_k(g, cyc) + 1 + 14 * d) % 16)

    def block_of(place, cyc, d, j):
        return plane_of(cyc, (ring_k(place, cyc) + 16 + (2 * d - 1) * j) % 16)

    def arrivals(place, j, count):
        slots = []
        for cyc in (0, 1):
            for d in (0, 1):
                src = block_of(place, cyc, d, j)
                on = 1 if d == 0 else jnp.logical_and(j > 0, j < 8).astype(jnp.int32)
                plain = (src < plain_nb).astype(jnp.int32)
                slots.append(plain * count + (1 - plain) * (2 * plain_nb + (src - plain_nb) * 2 + cyc))
                count = count + plain * on
        return slots, count

    barrier = pltpu.get_barrier_semaphore()
    nbr = [neighbour(cyc, d) for cyc in (0, 1) for d in (0, 1)]
    partners = [dev(t, n * 4 + x) for n in nbr]
    partners += [dev(t, g * 4 + (x + dx) % 4) for dx in (1, 2, 3)] + [dev(1 - t, c)]
    VTS[...] = cv_ref[...].T
    for p in partners:
        pl.semaphore_signal(barrier, inc=1, device_id=p, device_id_type=pl.DeviceIdType.MESH)
    pl.semaphore_wait(barrier, len(partners))

    def remote(src, dst, send, recv, device):
        return pltpu.make_async_remote_copy(src_ref=src, dst_ref=dst, send_sem=send, recv_sem=recv,
                                            device_id=device, device_id_type=pl.DeviceIdType.MESH)

    def q_cols(chip_x):
        return QT.at[:, :, pl.ds(pl.multiple_of(chip_x * COLS, 128), COLS)]

    def q_copy(dx, chip_x):
        return remote(qt_ref, q_cols(chip_x), q_send.at[dx - 1], q_recv.at[dx - 1], dev(t, g * 4 + (x + dx) % 4))

    def k_slot(slot):
        return KC.at[slot // 4, pl.ds(pl.multiple_of((slot % 4) * SLOTS, SLOTS), SLOTS), :]

    def v_slot(slot):
        return VC.at[slot // 4, :, pl.ds(pl.multiple_of((slot % 4) * SLOTS, SLOTS), SLOTS)]

    mine = pl.ds(pl.multiple_of(t * 128, 128), 128)
    other = pl.ds(pl.multiple_of((1 - t) * 128, 128), 128)
    own_slots, own_count = arrivals(g, 0, 0)
    own_slots = (own_slots[0], own_slots[2])

    def sib_copies(half):
        slot = own_slots[0] * (1 - half) + own_slots[1] * half
        return (remote(ck_ref.at[:, other], k_slot(slot), sib_send.at[0], sib_recv.at[0], dev(1 - t, c)),
                remote(VTS.at[other], v_slot(slot), sib_send.at[1], sib_recv.at[1], dev(1 - t, c)))

    my_slot = own_slots[0] * (1 - t) + own_slots[1] * t
    local = [pltpu.make_async_copy(qt_ref, q_cols(x), loc_sem.at[0]),
             pltpu.make_async_copy(kvn_ref, KVN.at[g], loc_sem.at[1])]
    local_cache = [pltpu.make_async_copy(ck_ref.at[:, mine], k_slot(my_slot), loc_sem.at[2]),
                   pltpu.make_async_copy(VTS.at[mine], v_slot(my_slot), loc_sem.at[3])]

    @pl.when(g < nb)
    def _():
        for cp in sib_copies(t):
            cp.start()
        for cp in local_cache:
            cp.start()
    for cp in local:
        cp.start()
    for dx in (2, 1, 3):
        q_copy(dx, x).start()

    def for_copies(s, fn, back, src_slots, dst_slots):
        for kind in range(3):
            for b in range(4):
                cyc, d = b // 2, b % 2
                place = block_of(g, cyc, d, s - back)
                live = s <= 8 - d
                if kind < 2:
                    live = jnp.logical_and(live, place < nb)

                @pl.when(live)
                def _():
                    if kind == 2:
                        src = dst = KVN.at[place, cyc]
                    else:
                        src, dst = [(k_slot, v_slot)[kind](v[b]) for v in (src_slots, dst_slots)]
                    fn(remote(src, dst, send_sem.at[b, kind, s], recv_sem.at[b, kind, s], dev(t, nbr[b] * 4 + x)))

    zero_slots = (0, 0, 0, 0)
    nbr_counts, first_slots = [], []
    for b in range(4):
        _, count = arrivals(nbr[b], 0, 0)
        slots, count = arrivals(nbr[b], 1, count)
        nbr_counts.append(count)
        first_slots.append(slots[b])

    for cp in local:
        cp.wait()

    @pl.when(g < nb)
    def _():
        for cp in local_cache:
            cp.wait()
        for cp in sib_copies(1 - t):
            cp.wait_recv()

    for_copies(1, lambda cp: cp.start(), 1, (own_slots[0], own_slots[0], own_slots[1], own_slots[1]), first_slots)

    ACC[:, 128:136, :] = jnp.where(lax.broadcasted_iota(jnp.int32, (2, 8, QW), 1) == 0, NEG, 0.0)
    ACC[:, 0:128, :] = jnp.zeros((2, 128, QW), jnp.float32)

    def units(half, key, val_t, mask):
        cols = [pl.ds(tile * 256, 256) for tile in range(6)]

        def score(i):
            s = jnp.dot(key, QT[half, :, cols[i]], preferred_element_type=jnp.float32)
            return s if mask is None else mask(i, s)

        scores = [score(0)] + [None] * 5
        probs = [None] * 6
        alphas = [None] * 6
        for i in range(7):
            if i < 5:
                scores[i + 1] = score(i + 1)
            if i < 6:
                col, s = cols[i], scores[i]
                old_max = ACC[half, 128:129, col]
                new_max = jnp.maximum(old_max, jnp.max(s, axis=0, keepdims=True))
                e = jnp.exp2(s * EXP_C - new_max * EXP_C)
                alphas[i] = jnp.exp2((old_max - new_max) * EXP_C)
                ACC[half, 128:129, col] = new_max
                ACC[half, 129:130, col] = ACC[half, 129:130, col] * alphas[i] + jnp.sum(e, axis=0, keepdims=True)
                probs[i] = e.astype(jnp.bfloat16)
            if i > 0:
                col = cols[i - 1]
                ACC[half, 0:128, col] = ACC[half, 0:128, col] * alphas[i - 1] + jnp.dot(
                    val_t, probs[i - 1], preferred_element_type=jnp.float32)

    for dx in (1, 3, 2):
        q_copy(dx, (x + 4 - dx) % 4).wait_recv()

    def plain_groups(first, last):
        def body(i, carry):
            units(i % 2, KC[i // 2], VC[i // 2], None)
            return carry
        lax.fori_loop(2 * first, 2 * last, body, 0)

    def step(s, carry):
        count, counts = carry[0], carry[1:]
        slots, new_count = arrivals(g, s, count)
        next_slots, new_counts = [], []
        for b in range(4):
            nxt, cnt = arrivals(nbr[b], s + 1, counts[b])
            next_slots.append(nxt[b])
            new_counts.append(cnt)
        for_copies(s, lambda cp: cp.wait_recv(), 0, zero_slots, zero_slots)
        for_copies(s + 1, lambda cp: cp.start(), 1, slots, next_slots)
        if plain_nb:
            plain_groups((count - (s == 1).astype(jnp.int32) * own_count) // 4, new_count // 4)
        return (new_count, *new_counts)

    lax.fori_loop(1, 9, step, (own_count + jnp.int32(0), *nbr_counts))

    def last_group(half, carry):
        row = lax.broadcasted_iota(jnp.int32, (4 * SLOTS, 1), 0)
        slot = (4 * (plain_nb + row // (2 * SLOTS)) + x) * (2 * SLOTS) + row % (2 * SLOTS)
        seen = slot < cache_len
        units(half, KC[nb // 2 - 1], VC[nb // 2 - 1], lambda i, s: jnp.where(seen, s, NEG))
        return carry

    lax.fori_loop(0, 2, last_group, 0)

    units(1, KVN[:, :, 0, 0].reshape(1024, 128), KVN[:, :, 1, 0].reshape(1024, 128).T, None)

    edge = g // 8

    def new_item(j, carry):
        late = (j > edge).astype(jnp.int32)
        blk = j - late
        places = pl.ds(blk * 8, 8)
        key = KVN[places, :, 0, late].reshape(512, 128)
        val_t = KVN[places, :, 1, late].reshape(512, 128).T
        row = lax.broadcasted_iota(jnp.int32, (512, 1), 0)
        run = 2 * (4 * (blk * 8 + row // 64) + x) + (row % 64) // 32
        key_pos = (run + late * (255 - 2 * run)) * 32 + row % 32

        def causal(i, s):
            col = lax.broadcasted_iota(jnp.int32, (1, 256), 1) + i * 256
            q_run = 2 * (4 * g + col // COLS) + (col % 64) // 32
            q_pos = (q_run + late * (255 - 2 * q_run)) * 32 + col % 32
            return jnp.where(key_pos <= q_pos, s, NEG)

        units(late, key, val_t, causal)
        return carry

    lax.fori_loop(0, 3, new_item, 0)

    def o_copy(dx):
        dst_x = (x + dx) % 4
        return remote(ACC.at[:, :, pl.ds(pl.multiple_of(dst_x * COLS, 128), COLS)], PART.at[dx - 1],
                      o_send.at[dx - 1], o_recv.at[dx - 1], dev(t, g * 4 + dst_x))

    for dx in (2, 1, 3):
        o_copy(dx).start()
    for dx in (1, 3, 2):
        o_copy(dx).wait_recv()
    own = pl.ds(pl.multiple_of(x * COLS, 128), COLS)
    for half in (0, 1):
        maxes = [ACC[half, 128:129, own]] + [PART[i, half, 128:129, :] for i in range(3)]
        sums = [ACC[half, 129:130, own]] + [PART[i, half, 129:130, :] for i in range(3)]
        top = functools.reduce(jnp.maximum, maxes)
        weights = [jnp.exp2((m - top) * EXP_C) for m in maxes]
        total = sum(w * l for w, l in zip(weights, sums))
        acc = ACC[half, 0:128, own] * weights[0]
        for i in range(3):
            acc = acc + PART[i, half, 0:128, :] * weights[i + 1]
        o_rows = (acc / total).T.astype(jnp.bfloat16)
        for head in range(HEADS):
            for core in (0, 1):
                out_ref[core * 64 + half * 32:core * 64 + half * 32 + 32, head * 128:head * 128 + 128] = \
                    o_rows[head * 64 + core * 32:head * 64 + core * 32 + 32, :]

    for dx in (1, 2, 3):
        q_copy(dx, x).wait_send()
        o_copy(dx).wait_send()

    @pl.when(g < nb)
    def _():
        for cp in sib_copies(t):
            cp.wait_send()

    def drain(s, carry):
        for_copies(s, lambda cp: cp.wait_send(), 1, zero_slots, zero_slots)
        return carry
    lax.fori_loop(1, 9, drain, 0)


def attend(index, cache_len, q_t, kv_new, cache_k, cache_v):
    nb = 2 * index + 2
    bf16, f32 = jnp.bfloat16, jnp.float32
    vmem = pl.BlockSpec(memory_space=pltpu.VMEM)
    return pl.pallas_call(
        functools.partial(attend_kernel, nb),
        out_shape=jax.ShapeDtypeStruct((128, HEADS * HEAD_DIM), bf16),
        in_specs=[pl.BlockSpec(memory_space=pltpu.SMEM), vmem, vmem, vmem, vmem],
        out_specs=vmem,
        scratch_shapes=[
            pltpu.VMEM((2, 128, QW), bf16),
            pltpu.VMEM((nb // 2, 4 * SLOTS, 128), bf16),
            pltpu.VMEM((nb // 2, 128, 4 * SLOTS), bf16),
            pltpu.VMEM((16, 2, 2, 2, 32, 128), bf16),
            pltpu.VMEM((2, 136, QW), f32),
            pltpu.VMEM((3, 2, 136, COLS), f32),
            pltpu.VMEM((256, SLOTS), bf16),
            pltpu.SemaphoreType.DMA((4, 3, 9)),
            pltpu.SemaphoreType.DMA((4, 3, 9)),
            pltpu.SemaphoreType.DMA((3,)),
            pltpu.SemaphoreType.DMA((3,)),
            pltpu.SemaphoreType.DMA((3,)),
            pltpu.SemaphoreType.DMA((3,)),
            pltpu.SemaphoreType.DMA((2,)),
            pltpu.SemaphoreType.DMA((2,)),
            pltpu.SemaphoreType.DMA((4,)),
        ],
        compiler_params=pltpu.CompilerParams(collective_id=index, has_side_effects=True, vmem_limit_bytes=56 * 1024 * 1024),
        name='attend_%d' % nb,
    )(cache_len, q_t, kv_new, cache_k, cache_v)


def solution(mesh):
    token_spec = P(('dp', 'cp', 'tp'), None)
    column_spec = P(None, 'tp')
    row_spec = P('tp', None)

    def device_layer(hidden_loc, pos_loc, cache_len, cache_k, cache_v, norm1_gain, w_query, w_key, w_value, w_out, norm2_gain, w_gate, w_up, w_down):
        normed = rms_norm(hidden_loc, norm1_gain)
        group_in = lax.all_gather(normed, 'tp', axis=0, tiled=True)
        rows = group_in.shape[0]
        row = jnp.arange(rows, dtype=jnp.int32)
        run = 2 * lax.axis_index('cp') + row // 64
        run = jnp.where(row % 64 < 32, run, 255 - run)
        group_pos = cache_len[0] + run * 32 + row % 32
        queries = rotary(jnp.dot(group_in, w_query, preferred_element_type=jnp.float32).reshape(rows, HEADS, HEAD_DIM), group_pos)
        keys_new = rotary(jnp.dot(group_in, w_key, preferred_element_type=jnp.float32), group_pos)
        values_new = jnp.dot(group_in, w_value, preferred_element_type=jnp.float32).astype(jnp.bfloat16)
        q_t = jnp.transpose(queries.reshape(2, 2, 32, HEADS, HEAD_DIM), (1, 4, 3, 0, 2)).reshape(2, HEAD_DIM, COLS)
        kv_new = jnp.stack([keys_new.reshape(2, 2, 32, HEAD_DIM), values_new.reshape(2, 2, 32, HEAD_DIM)], axis=1)
        bucket = jnp.clip((cache_len[0] - 1) // (16 * SLOTS), 0, BUCKETS - 1)
        attended = lax.switch(bucket, [functools.partial(attend, i) for i in range(BUCKETS)], cache_len, q_t, kv_new, cache_k, cache_v)
        attn_part = jnp.dot(attended, w_out, preferred_element_type=jnp.float32)
        residual_mid = (hidden_loc.astype(jnp.float32) + lax.psum_scatter(attn_part, 'tp', scatter_dimension=0, tiled=True)).astype(jnp.bfloat16)
        group_mid = lax.all_gather(rms_norm(residual_mid, norm2_gain), 'tp', axis=0, tiled=True)
        gate_proj = jnp.dot(group_mid, w_gate, preferred_element_type=jnp.float32)
        up_proj = jnp.dot(group_mid, w_up, preferred_element_type=jnp.float32)
        hidden_mlp = (jax.nn.silu(gate_proj) * up_proj).astype(jnp.bfloat16)
        mlp_part = jnp.dot(hidden_mlp, w_down, preferred_element_type=jnp.float32)
        return (residual_mid.astype(jnp.float32) + lax.psum_scatter(mlp_part, 'tp', scatter_dimension=0, tiled=True)).astype(jnp.bfloat16)

    return jax.shard_map(device_layer, mesh=mesh, in_specs=(token_spec, P(('dp', 'cp', 'tp')), P('dp'), token_spec, token_spec, P(), column_spec, column_spec, column_spec, row_spec, P(), column_spec, column_spec, row_spec), out_specs=token_spec, check_vma=False)
```

```python
import functools
import math
import jax
import jax.numpy as jnp
from jax import lax
from jax.experimental import pallas as pl
from jax.experimental.pallas import tpu as pltpu
from jax.sharding import PartitionSpec as P

HEAD_DIM = 128
ROPE_BASE = 500000.0
NORM_EPS = 1e-5
HEADS = 6
SLOTS = 256
COLS = HEADS * 128
GROUP = 4 * SLOTS
FFN_TILE = 896
NEG = -2.3e38
EXP_C = math.log2(math.e) / math.sqrt(HEAD_DIM)
BUCKETS = 4
MASKED = 8 // BUCKETS


def rms_norm(hidden, norm_gain):
    values = hidden.astype(jnp.float32)
    inv_rms = lax.rsqrt(jnp.mean(values * values, axis=-1, keepdims=True) + NORM_EPS)
    return (values * inv_rms * norm_gain.astype(jnp.float32)).astype(jnp.bfloat16)


def rotary(projected, positions):
    half_dim = HEAD_DIM // 2
    inv_freq = 1.0 / (ROPE_BASE ** (jnp.arange(half_dim, dtype=jnp.float32) * (2.0 / HEAD_DIM)))
    angles = positions.astype(jnp.float32)[:, None] * inv_freq[None, :]
    expand = (angles.shape[0],) + (1,) * (projected.ndim - 2) + (half_dim,)
    cos_table = jnp.cos(angles).reshape(expand)
    sin_table = jnp.sin(angles).reshape(expand)
    first_half = projected[..., :half_dim]
    second_half = projected[..., half_dim:]
    rotated = jnp.concatenate([first_half * cos_table - second_half * sin_table, second_half * cos_table + first_half * sin_table], axis=-1)
    return rotated.astype(jnp.bfloat16)


def plane_of(cyc, k):
    major = k // 4
    minor = (k - major) % 4
    return (4 * major + minor) * (1 - cyc) + (4 * minor + major) * cyc


def attend_kernel(nb, len_ref, qt_ref, kvn_ref, ck_ref, cv_ref, out_ref,
                  QT, KC, VC, KVN, ACC, PART, VTS, KPOS,
                  send_sem, recv_sem, q_send, q_recv, o_send, o_recv, sib_send, sib_recv, loc_sem):
    c = lax.axis_index('cp')
    t = lax.axis_index('tp')
    x = c % 4
    g = c // 4
    cache_len = len_ref[0]
    plain_nb = nb - 2 * MASKED

    def dev(core, chip):
        return {'tp': core, 'cp': chip}

    def ring_k(place, cyc):
        zz, yy = place // 4, place % 4
        return (4 * zz) * (1 - cyc) + (4 * yy) * cyc + (yy + zz) % 4

    def neighbour(cyc, d):
        return plane_of(cyc, (ring_k(g, cyc) + 1 + 14 * d) % 16)

    def block_of(place, cyc, d, j):
        return plane_of(cyc, (ring_k(place, cyc) + 16 + (2 * d - 1) * j) % 16)

    def arrivals(place, j, count):
        slots = []
        for cyc in (0, 1):
            for d in (0, 1):
                src = block_of(place, cyc, d, j)
                on = 1 if d == 0 else jnp.logical_and(j > 0, j < 8).astype(jnp.int32)
                plain = (src < plain_nb).astype(jnp.int32)
                slots.append(plain * count + (1 - plain) * (2 * plain_nb + (src - plain_nb) * 2 + cyc))
                count = count + plain * on
        return slots, count

    barrier = pltpu.get_barrier_semaphore()
    nbr = [neighbour(cyc, d) for cyc in (0, 1) for d in (0, 1)]
    partners = [dev(t, n * 4 + x) for n in nbr]
    partners += [dev(t, g * 4 + (x + dx) % 4) for dx in (1, 2, 3)] + [dev(1 - t, c)]
    VTS[...] = cv_ref[...].T
    for p in partners:
        pl.semaphore_signal(barrier, inc=1, device_id=p, device_id_type=pl.DeviceIdType.MESH)
    pl.semaphore_wait(barrier, len(partners))

    def remote(src, dst, send, recv, device):
        return pltpu.make_async_remote_copy(src_ref=src, dst_ref=dst, send_sem=send, recv_sem=recv,
                                            device_id=device, device_id_type=pl.DeviceIdType.MESH)

    def q_copy(dx, chip_x):
        return remote(qt_ref, QT.at[chip_x], q_send.at[dx - 1], q_recv.at[dx - 1], dev(t, g * 4 + (x + dx) % 4))

    def k_slot(slot):
        return KC.at[slot // 4, pl.ds(pl.multiple_of((slot % 4) * SLOTS, SLOTS), SLOTS), :]

    def v_slot(slot):
        return VC.at[slot // 4, :, pl.ds(pl.multiple_of((slot % 4) * SLOTS, SLOTS), SLOTS)]

    mine = pl.ds(pl.multiple_of(t * 128, 128), 128)
    other = pl.ds(pl.multiple_of((1 - t) * 128, 128), 128)
    own_slots, own_count = arrivals(g, 0, 0)
    own_slots = (own_slots[0], own_slots[2])

    def sib_copies(half):
        slot = own_slots[0] * (1 - half) + own_slots[1] * half
        return (remote(ck_ref.at[:, other], k_slot(slot), sib_send.at[0], sib_recv.at[0], dev(1 - t, c)),
                remote(VTS.at[other], v_slot(slot), sib_send.at[1], sib_recv.at[1], dev(1 - t, c)))

    my_slot = own_slots[0] * (1 - t) + own_slots[1] * t
    local = [pltpu.make_async_copy(qt_ref, QT.at[x], loc_sem.at[0]),
             pltpu.make_async_copy(kvn_ref, KVN.at[g], loc_sem.at[1])]
    local_cache = [pltpu.make_async_copy(ck_ref.at[:, mine], k_slot(my_slot), loc_sem.at[2]),
                   pltpu.make_async_copy(VTS.at[mine], v_slot(my_slot), loc_sem.at[3])]

    @pl.when(g < nb)
    def _():
        for cp in sib_copies(t):
            cp.start()
        for cp in local_cache:
            cp.start()
    for cp in local:
        cp.start()
    for dx in (2, 1, 3):
        q_copy(dx, x).start()

    def for_copies(s, fn, back, src_slots, dst_slots):
        for kind in range(3):
            for b in range(4):
                cyc, d = b // 2, b % 2
                place = block_of(g, cyc, d, s - back)
                live = s <= 8 - d
                if kind < 2:
                    live = jnp.logical_and(live, place < nb)

                @pl.when(live)
                def _():
                    if kind == 2:
                        src = dst = KVN.at[place, cyc]
                    else:
                        src, dst = [(k_slot, v_slot)[kind](v[b]) for v in (src_slots, dst_slots)]
                    fn(remote(src, dst, send_sem.at[b, kind, s], recv_sem.at[b, kind, s], dev(t, nbr[b] * 4 + x)))

    zero_slots = (0, 0, 0, 0)
    nbr_counts, first_slots = [], []
    for b in range(4):
        _, count = arrivals(nbr[b], 0, 0)
        slots, count = arrivals(nbr[b], 1, count)
        nbr_counts.append(count)
        first_slots.append(slots[b])

    for cp in local:
        cp.wait()

    @pl.when(g < nb)
    def _():
        for cp in local_cache:
            cp.wait()
        for cp in sib_copies(1 - t):
            cp.wait_recv()

    for_copies(1, lambda cp: cp.start(), 1, (own_slots[0], own_slots[0], own_slots[1], own_slots[1]), first_slots)

    ACC[:, 128:136, :] = jnp.where(lax.broadcasted_iota(jnp.int32, (4, 8, COLS), 1) == 0, NEG, 0.0)
    ACC[:, 0:128, :] = jnp.zeros((4, 128, COLS), jnp.float32)
    row = lax.broadcasted_iota(jnp.int32, (GROUP, 128), 0)
    run = 2 * (4 * (row // 64) + x) + (row % 64) // 32
    for i in range(MASKED):
        slot_id = (4 * (plain_nb + 2 * i + row // (2 * SLOTS)) + x) * (2 * SLOTS) + row % (2 * SLOTS)
        KPOS[i] = jnp.where(slot_id < cache_len, -1, 1 << 30)
    KPOS[MASKED] = run * 32 + row % 32
    KPOS[MASKED + 1] = (255 - run) * 32 + row % 32

    def units(group, chip, masked):
        cols = [pl.ds(tile * 256, 256) for tile in range(3)]
        key, val_t = KC[group], VC[group]

        def score(i):
            s = jnp.dot(key, QT[chip, :, cols[i]], preferred_element_type=jnp.float32)
            if masked:
                col = lax.broadcasted_iota(jnp.int32, (1, 256), 1) + i * 256
                late = col // (COLS // 2)
                q_run = 2 * (4 * g + chip) + (col % 64) // 32
                q_pos = (q_run + late * (255 - 2 * q_run)) * 32 + col % 32
                k_pos = KPOS[group - plain_nb // 2]
                seen = [k_pos <= q_pos[:, :128], k_pos <= q_pos[:, 128:]]
                s = jnp.concatenate([jnp.where(seen[j], s[:, j * 128:j * 128 + 128], NEG) for j in (0, 1)], axis=1)
            return s

        scores = [score(0)] + [None] * 2
        probs = [None] * 3
        alphas = [None] * 3
        for i in range(4):
            if i < 2:
                scores[i + 1] = score(i + 1)
            if i < 3:
                col, s = cols[i], scores[i]
                old_max = ACC[chip, 128:129, col]
                new_max = jnp.maximum(old_max, jnp.max(s, axis=0, keepdims=True))
                e = jnp.exp2(s * EXP_C - new_max * EXP_C)
                alphas[i] = jnp.exp2((old_max - new_max) * EXP_C)
                ACC[chip, 128:129, col] = new_max
                ACC[chip, 129:130, col] = ACC[chip, 129:130, col] * alphas[i] + jnp.sum(e, axis=0, keepdims=True)
                probs[i] = e.astype(jnp.bfloat16)
            if i > 0:
                col = cols[i - 1]
                ACC[chip, 0:128, col] = ACC[chip, 0:128, col] * alphas[i - 1] + jnp.dot(
                    val_t, probs[i - 1], preferred_element_type=jnp.float32)

    for dx in (1, 3, 2):
        q_copy(dx, (x + 4 - dx) % 4).wait_recv()

    def o_copy(dx):
        dst_x = (x + dx) % 4
        return remote(ACC.at[dst_x], PART.at[dx - 1], o_send.at[dx - 1], o_recv.at[dx - 1], dev(t, g * 4 + dst_x))

    groups = plain_nb // 2

    def step(s, carry):
        count, early, counts = carry[0], carry[1], carry[2:]
        slots, new_count = arrivals(g, s, count)
        next_slots, new_counts = [], []
        for b in range(4):
            nxt, cnt = arrivals(nbr[b], s + 1, counts[b])
            next_slots.append(nxt[b])
            new_counts.append(cnt)
        ring = s <= 8
        for_copies(s, lambda cp: cp.wait_recv(), 0, zero_slots, zero_slots)
        for_copies(s + 1, lambda cp: cp.start(), 1, slots, next_slots)
        phase = s - 9
        dx = jnp.where(phase == 0, 2, jnp.where(phase == 1, 1, jnp.where(phase == 2, 3, 0)))

        @pl.when(s == 9)
        def _():
            for part in (0, 1):
                KC[groups + MASKED + part] = KVN[:, :, 0, part].reshape(GROUP, 128)
                VC[groups + MASKED + part] = KVN[:, :, 1, part].reshape(GROUP, 128).T

        @pl.when(s == 10)
        def _():
            o_copy(2).start()

        @pl.when(s == 11)
        def _():
            o_copy(1).start()

        @pl.when(s == 12)
        def _():
            o_copy(3).start()

        new_early = jnp.where(s < 8, new_count // 4, early)
        first = jnp.where(ring, 4 * early, 0)
        last = jnp.where(ring, 4 * new_early, groups - early)

        def plain(n, inner):
            units(jnp.where(ring, n // 4, early + n), jnp.where(ring, n % 4, (x + dx) % 4), False)
            return inner
        lax.fori_loop(first, last, plain, 0)

        def masked(n, inner):
            units(groups + n, (x + dx) % 4, True)
            return inner
        lax.fori_loop(0, jnp.where(ring, 0, MASKED + 2), masked, 0)
        return (jnp.where(ring, new_count, count), new_early, *new_counts)

    lax.fori_loop(1, 13, step, (own_count + jnp.int32(0), jnp.int32(0), *nbr_counts))

    for dx in (1, 3, 2):
        o_copy(dx).wait_recv()
    maxes = [ACC[x, 128:129, :]] + [PART[i, 128:129, :] for i in range(3)]
    sums = [ACC[x, 129:130, :]] + [PART[i, 129:130, :] for i in range(3)]
    top = functools.reduce(jnp.maximum, maxes)
    weights = [jnp.exp2((m - top) * EXP_C) for m in maxes]
    total = sum(w * l for w, l in zip(weights, sums))
    acc = ACC[x, 0:128, :] * weights[0]
    for i in range(3):
        acc = acc + PART[i, 0:128, :] * weights[i + 1]
    o_rows = (acc / total).T.astype(jnp.bfloat16)
    for half in (0, 1):
        for head in range(HEADS):
            for core in (0, 1):
                base = half * (COLS // 2) + head * 64 + core * 32
                out_ref[core * 64 + half * 32:core * 64 + half * 32 + 32, head * 128:head * 128 + 128] = o_rows[base:base + 32, :]

    for dx in (1, 2, 3):
        q_copy(dx, x).wait_send()
        o_copy(dx).wait_send()

    @pl.when(g < nb)
    def _():
        for cp in sib_copies(t):
            cp.wait_send()

    def drain(s, carry):
        for_copies(s, lambda cp: cp.wait_send(), 1, zero_slots, zero_slots)
        return carry
    lax.fori_loop(1, 9, drain, 0)


def attend(index, cache_len, q_t, kv_new, cache_k, cache_v):
    nb = (index + 1) * 16 // BUCKETS
    bf16, f32 = jnp.bfloat16, jnp.float32
    vmem = pl.BlockSpec(memory_space=pltpu.VMEM)
    return pl.pallas_call(
        functools.partial(attend_kernel, nb),
        out_shape=jax.ShapeDtypeStruct((128, HEADS * HEAD_DIM), bf16),
        in_specs=[pl.BlockSpec(memory_space=pltpu.SMEM), vmem, vmem, vmem, vmem],
        out_specs=vmem,
        scratch_shapes=[
            pltpu.VMEM((4, 128, COLS), bf16),
            pltpu.VMEM((nb // 2 + 2, GROUP, 128), bf16),
            pltpu.VMEM((nb // 2 + 2, 128, GROUP), bf16),
            pltpu.VMEM((16, 2, 2, 2, 32, 128), bf16),
            pltpu.VMEM((4, 136, COLS), f32),
            pltpu.VMEM((3, 136, COLS), f32),
            pltpu.VMEM((256, SLOTS), bf16),
            pltpu.VMEM((MASKED + 2, GROUP, 128), jnp.int32),
            pltpu.SemaphoreType.DMA((4, 3, 9)),
            pltpu.SemaphoreType.DMA((4, 3, 9)),
            pltpu.SemaphoreType.DMA((3,)),
            pltpu.SemaphoreType.DMA((3,)),
            pltpu.SemaphoreType.DMA((3,)),
            pltpu.SemaphoreType.DMA((3,)),
            pltpu.SemaphoreType.DMA((2,)),
            pltpu.SemaphoreType.DMA((2,)),
            pltpu.SemaphoreType.DMA((4,)),
        ],
        compiler_params=pltpu.CompilerParams(collective_id=index, has_side_effects=True, vmem_limit_bytes=56 * 1024 * 1024),
        name='attend_%d' % nb,
    )(cache_len, q_t, kv_new, cache_k, cache_v)


def tail_kernel(att_ref, hid_ref, gain_ref, wo_hbm, wg_hbm, wu_hbm, wd_hbm, out_ref,
                WO, WG, WU, WD, PARTS, GOT, NORM, HM, w_sem, send_sem, recv_sem):
    c = lax.axis_index('cp')
    t = lax.axis_index('tp')
    tiles = WG.shape[0]
    sibling = {'tp': 1 - t, 'cp': c}

    def load_out():
        return pltpu.make_async_copy(wo_hbm, WO, w_sem.at[0, 0])

    def load_in(i):
        cols = pl.ds(i * FFN_TILE, FFN_TILE)
        return (pltpu.make_async_copy(wg_hbm.at[:, cols], WG.at[i], w_sem.at[1, i]),
                pltpu.make_async_copy(wu_hbm.at[:, cols], WU.at[i], w_sem.at[2, i]))

    def load_down(i):
        return pltpu.make_async_copy(wd_hbm.at[pl.ds(i * FFN_TILE, FFN_TILE), :], WD.at[i], w_sem.at[3, i])

    load_out().start()
    for i in range(tiles):
        for cp in load_in(i):
            cp.start()
    for i in range(tiles):
        load_down(i).start()
    barrier = pltpu.get_barrier_semaphore()
    pl.semaphore_signal(barrier, inc=1, device_id=sibling, device_id_type=pl.DeviceIdType.MESH)
    pl.semaphore_wait(barrier, 1)

    def remote(src, dst, i):
        return pltpu.make_async_remote_copy(src_ref=src, dst_ref=dst, send_sem=send_sem.at[i], recv_sem=recv_sem.at[i],
                                            device_id=sibling, device_id_type=pl.DeviceIdType.MESH)

    mine = pl.ds(pl.multiple_of(t * 64, 64), 64)
    other = pl.ds(pl.multiple_of((1 - t) * 64, 64), 64)

    def add_over_cores(i, part):
        PARTS[i] = part
        copy = remote(PARTS.at[i, other], GOT.at[i], i)
        copy.start()
        copy.wait()
        return PARTS[i, mine, :] + GOT[i]

    load_out().wait()
    mid = (hid_ref[...].astype(jnp.float32)
           + add_over_cores(0, jnp.dot(att_ref[...], WO[...], preferred_element_type=jnp.float32))).astype(jnp.bfloat16)
    wide = mid.astype(jnp.float32)
    inv_rms = lax.rsqrt(jnp.mean(wide * wide, axis=-1, keepdims=True) + NORM_EPS)
    NORM[mine, :] = (wide * inv_rms * gain_ref[...].astype(jnp.float32)).astype(jnp.bfloat16)
    share = remote(NORM.at[mine], NORM.at[mine], 2)
    share.start()
    remote(NORM.at[other], NORM.at[other], 2).wait_recv()
    share.wait_send()

    for i in range(tiles):
        for cp in load_in(i):
            cp.wait()
        gate = jnp.dot(NORM[...], WG[i], preferred_element_type=jnp.float32)
        up = jnp.dot(NORM[...], WU[i], preferred_element_type=jnp.float32)
        HM[i] = (gate * jax.nn.sigmoid(gate) * up).astype(jnp.bfloat16)
    total = None
    for i in range(tiles):
        load_down(i).wait()
        part = jnp.dot(HM[i], WD[i], preferred_element_type=jnp.float32)
        total = part if total is None else total + part
    out_ref[...] = (wide + add_over_cores(1, total)).astype(jnp.bfloat16)


def mlp_tail(attended, hidden, gain, w_out, w_gate, w_up, w_down):
    bf16, f32 = jnp.bfloat16, jnp.float32
    width, ffn = w_gate.shape
    tiles = ffn // FFN_TILE
    vmem = pl.BlockSpec(memory_space=pltpu.VMEM)
    hbm = pl.BlockSpec(memory_space=pl.ANY)
    return pl.pallas_call(
        tail_kernel,
        out_shape=jax.ShapeDtypeStruct(hidden.shape, bf16),
        in_specs=[vmem, vmem, vmem, hbm, hbm, hbm, hbm],
        out_specs=vmem,
        scratch_shapes=[
            pltpu.VMEM(w_out.shape, bf16),
            pltpu.VMEM((tiles, width, FFN_TILE), bf16),
            pltpu.VMEM((tiles, width, FFN_TILE), bf16),
            pltpu.VMEM((tiles, FFN_TILE, width), bf16),
            pltpu.VMEM((2, 128, width), f32),
            pltpu.VMEM((2, 64, width), f32),
            pltpu.VMEM((128, width), bf16),
            pltpu.VMEM((tiles, 128, FFN_TILE), bf16),
            pltpu.SemaphoreType.DMA((4, tiles)),
            pltpu.SemaphoreType.DMA((3,)),
            pltpu.SemaphoreType.DMA((3,)),
        ],
        compiler_params=pltpu.CompilerParams(collective_id=BUCKETS, has_side_effects=True, vmem_limit_bytes=62 * 1024 * 1024),
        name='mlp_tail',
    )(attended, hidden, gain.reshape(1, -1), w_out, w_gate, w_up, w_down)


def solution(mesh):
    token_spec = P(('dp', 'cp', 'tp'), None)
    column_spec = P(None, 'tp')
    row_spec = P('tp', None)

    def device_layer(hidden_loc, pos_loc, cache_len, cache_k, cache_v, norm1_gain, w_query, w_key, w_value, w_out, norm2_gain, w_gate, w_up, w_down):
        normed = rms_norm(hidden_loc, norm1_gain)
        group_in = lax.all_gather(normed, 'tp', axis=0, tiled=True)
        rows = group_in.shape[0]
        row = jnp.arange(rows, dtype=jnp.int32)
        run = 2 * lax.axis_index('cp') + row // 64
        run = jnp.where(row % 64 < 32, run, 255 - run)
        group_pos = cache_len[0] + run * 32 + row % 32
        queries = rotary(jnp.dot(group_in, w_query, preferred_element_type=jnp.float32).reshape(rows, HEADS, HEAD_DIM), group_pos)
        keys_new = rotary(jnp.dot(group_in, w_key, preferred_element_type=jnp.float32), group_pos)
        values_new = jnp.dot(group_in, w_value, preferred_element_type=jnp.float32).astype(jnp.bfloat16)
        q_t = jnp.transpose(queries.reshape(2, 2, 32, HEADS, HEAD_DIM), (4, 1, 3, 0, 2)).reshape(HEAD_DIM, COLS)
        kv_new = jnp.stack([keys_new.reshape(2, 2, 32, HEAD_DIM), values_new.reshape(2, 2, 32, HEAD_DIM)], axis=1)
        bucket = jnp.clip((cache_len[0] - 1) // (128 * SLOTS // BUCKETS), 0, BUCKETS - 1)
        attended = lax.switch(bucket, [functools.partial(attend, i) for i in range(BUCKETS)], cache_len, q_t, kv_new, cache_k, cache_v)
        return mlp_tail(attended, hidden_loc, norm2_gain, w_out, w_gate, w_up, w_down)

    return jax.shard_map(device_layer, mesh=mesh, in_specs=(token_spec, P(('dp', 'cp', 'tp')), P('dp'), token_spec, token_spec, P(), column_spec, column_spec, column_spec, row_spec, P(), column_spec, column_spec, row_spec), out_specs=token_spec, check_vma=False)
```

```python
import functools
import math
import jax
import jax.numpy as jnp
from jax import lax
from jax.experimental import pallas as pl
from jax.experimental.pallas import tpu as pltpu
from jax.sharding import PartitionSpec as P

HEAD_DIM = 128
ROPE_BASE = 500000.0
NORM_EPS = 1e-5
HEADS = 6
SLOTS = 256
COLS = HEADS * 128
GROUP = 4 * SLOTS
FFN_TILE = 896
WARM = 3
NEG = -2.3e38
EXP_C = math.log2(math.e) / math.sqrt(HEAD_DIM)
BUCKETS = 4
MASKED = 8 // BUCKETS


def rotary_table(positions):
    half_dim = HEAD_DIM // 2
    inv_freq = 1.0 / (ROPE_BASE ** (jnp.arange(half_dim, dtype=jnp.float32) * (2.0 / HEAD_DIM)))
    angles = positions.astype(jnp.float32)[:, None] * inv_freq[None, :]
    cos_table, sin_table = jnp.cos(angles), jnp.sin(angles)
    return jnp.stack([jnp.concatenate([cos_table, cos_table], axis=1), jnp.concatenate([-sin_table, sin_table], axis=1)])


def plane_of(cyc, k):
    major = k // 4
    minor = (k - major) % 4
    return (4 * major + minor) * (1 - cyc) + (4 * minor + major) * cyc


def layer_kernel(nb, len_ref, table_ref, hid_ref, gain_ref, ck_ref, cv_ref,
                 wq_hbm, wk_hbm, wv_hbm, wo_hbm, wg_hbm, wu_hbm, wd_hbm, out_ref,
                 QT, KC, VC, KVN, ACC, PART, VTS, KPOS, WO, WG, WU, WD, NORM, SUM, GOT, HM,
                 send_sem, recv_sem, q_send, q_recv, o_send, o_recv, sib_send, sib_recv, loc_sem, w_sem, x_send, x_recv):
    c = lax.axis_index('cp')
    t = lax.axis_index('tp')
    x = c % 4
    g = c // 4
    cache_len = len_ref[0]
    plain_nb = nb - 2 * MASKED

    def dev(core, chip):
        return {'tp': core, 'cp': chip}

    def ring_k(place, cyc):
        zz, yy = place // 4, place % 4
        return (4 * zz) * (1 - cyc) + (4 * yy) * cyc + (yy + zz) % 4

    def neighbour(cyc, d):
        return plane_of(cyc, (ring_k(g, cyc) + 1 + 14 * d) % 16)

    def block_of(place, cyc, d, j):
        return plane_of(cyc, (ring_k(place, cyc) + 16 + (2 * d - 1) * j) % 16)

    def arrivals(place, j, count):
        slots = []
        for cyc in (0, 1):
            for d in (0, 1):
                src = block_of(place, cyc, d, j)
                on = 1 if d == 0 else jnp.logical_and(j > 0, j < 8).astype(jnp.int32)
                plain = (src < plain_nb).astype(jnp.int32)
                slots.append(plain * count + (1 - plain) * (2 * plain_nb + (src - plain_nb) * 2 + cyc))
                count = count + plain * on
        return slots, count

    barrier = pltpu.get_barrier_semaphore()
    nbr = [neighbour(cyc, d) for cyc in (0, 1) for d in (0, 1)]
    partners = [dev(t, n * 4 + x) for n in nbr]
    partners += [dev(t, g * 4 + (x + dx) % 4) for dx in (1, 2, 3)] + [dev(1 - t, c)]
    for p in partners:
        pl.semaphore_signal(barrier, inc=1, device_id=p, device_id_type=pl.DeviceIdType.MESH)

    tiles = WG.shape[0]

    def load_in(i):
        cols = pl.ds(pl.multiple_of(i * FFN_TILE, 128), FFN_TILE)
        return (pltpu.make_async_copy(wg_hbm.at[:, cols], WG.at[i], w_sem.at[1, i]),
                pltpu.make_async_copy(wu_hbm.at[:, cols], WU.at[i], w_sem.at[2, i]))

    def load_down(i):
        return pltpu.make_async_copy(wd_hbm.at[pl.ds(i * FFN_TILE, FFN_TILE), :], WD.at[i], w_sem.at[3, i])

    WQ = WG.at[tiles - 1, :, 0:HEADS * HEAD_DIM]
    WK, WV = WU.at[tiles - 1, :, 0:128], WU.at[tiles - 1, :, 128:256]
    load_qkv = [pltpu.make_async_copy(wk_hbm, WK, w_sem.at[0, 0]), pltpu.make_async_copy(wv_hbm, WV, w_sem.at[0, 1]),
                pltpu.make_async_copy(wq_hbm, WQ, w_sem.at[0, 2])]
    load_out = pltpu.make_async_copy(wo_hbm, WO, w_sem.at[0, 3])
    for cp in load_qkv:
        cp.start()
    load_out.start()
    for i in range(tiles - 1):
        for cp in load_in(i):
            cp.start()
    for i in range(tiles):
        load_down(i).start()

    my_rows = pl.ds(pl.multiple_of(t * 64, 64), 64)
    their_rows = pl.ds(pl.multiple_of((1 - t) * 64, 64), 64)

    def normed(i, values):
        inv_rms = lax.rsqrt(jnp.mean(values * values, axis=-1, keepdims=True) + NORM_EPS)
        NORM[i, my_rows, :] = (values * inv_rms * gain_ref[i:i + 1, :].astype(jnp.float32)).astype(jnp.bfloat16)

    VTS[...] = cv_ref[...].T
    normed(0, hid_ref[...].astype(jnp.float32))
    pl.semaphore_wait(barrier, len(partners))

    def remote(src, dst, send, recv, device):
        return pltpu.make_async_remote_copy(src_ref=src, dst_ref=dst, send_sem=send, recv_sem=recv,
                                            device_id=device, device_id_type=pl.DeviceIdType.MESH)

    def q_copy(dx, chip_x):
        return remote(QT.at[x], QT.at[chip_x], q_send.at[dx - 1], q_recv.at[dx - 1], dev(t, g * 4 + (x + dx) % 4))

    def k_slot(slot):
        return KC.at[slot // 4, pl.ds(pl.multiple_of((slot % 4) * SLOTS, SLOTS), SLOTS), :]

    def v_slot(slot):
        return VC.at[slot // 4, :, pl.ds(pl.multiple_of((slot % 4) * SLOTS, SLOTS), SLOTS)]

    mine = pl.ds(pl.multiple_of(t * 128, 128), 128)
    other = pl.ds(pl.multiple_of((1 - t) * 128, 128), 128)
    own_slots, own_count = arrivals(g, 0, 0)
    own_slots = (own_slots[0], own_slots[2])

    def sib_copies(half):
        slot = own_slots[0] * (1 - half) + own_slots[1] * half
        return (remote(ck_ref.at[:, other], k_slot(slot), sib_send.at[0], sib_recv.at[0], dev(1 - t, c)),
                remote(VTS.at[other], v_slot(slot), sib_send.at[1], sib_recv.at[1], dev(1 - t, c)))

    my_slot = own_slots[0] * (1 - t) + own_slots[1] * t
    local_cache = [pltpu.make_async_copy(ck_ref.at[:, mine], k_slot(my_slot), loc_sem.at[0]),
                   pltpu.make_async_copy(VTS.at[mine], v_slot(my_slot), loc_sem.at[1])]

    def share_norm(i):
        rows = NORM.at[i, my_rows]
        return remote(rows, rows, x_send.at[i], x_recv.at[i], dev(1 - t, c))

    def norm_landed(i):
        rows = NORM.at[i, their_rows]
        return remote(rows, rows, x_send.at[i], x_recv.at[i], dev(1 - t, c))

    share_norm(0).start()

    @pl.when(g < nb)
    def _():
        for cp in sib_copies(t):
            cp.start()
        for cp in local_cache:
            cp.start()

    def ring_copy(b, kind, s, place, src_slots, dst_slots):
        if kind == 2:
            src = dst = KVN.at[place, b // 2]
        else:
            src, dst = [(k_slot, v_slot)[kind](v[b]) for v in (src_slots, dst_slots)]
        return remote(src, dst, send_sem.at[b, kind, s], recv_sem.at[b, kind, s], dev(t, nbr[b] * 4 + x))

    def for_blocks(s, kinds, fn):
        for kind in kinds:
            for b in range(4):
                place = block_of(g, b // 2, b % 2, s)

                def run():
                    fn(b, kind, place)

                if kind < 2:
                    pl.when(place < nb)(run)
                else:
                    run()

    zero_slots = (0, 0, 0, 0)
    nbr_counts, first_slots = [], []
    for b in range(4):
        _, count = arrivals(nbr[b], 0, 0)
        slots, count = arrivals(nbr[b], 1, count)
        nbr_counts.append(count)
        first_slots.append(slots[b])

    own_four = (own_slots[0], own_slots[0], own_slots[1], own_slots[1])

    def first_sends(kinds):
        for_blocks(0, kinds, lambda b, kind, place: ring_copy(b, kind, 1, place, own_four, first_slots).start())

    @pl.when(g < nb)
    def _():
        for cp in local_cache:
            cp.wait()
        for cp in sib_copies(1 - t):
            cp.wait_recv()

    first_sends((0, 1))

    norm_landed(0).wait_recv()

    def project(weight):
        return jnp.dot(NORM[0], weight, preferred_element_type=jnp.float32)

    def rotated(head):
        return (head * table_ref[0] + pltpu.roll(head, 64, 1) * table_ref[1]).astype(jnp.bfloat16)

    for cp in load_qkv[:2]:
        cp.wait()
    new_kv = (rotated(project(WK[...])), project(WV[...]).astype(jnp.bfloat16))
    for kv in (0, 1):
        for core in (0, 1):
            for half in (0, 1):
                base = core * 64 + half * 32
                KVN[g, core, kv, half] = new_kv[kv][base:base + 32, :]
    load_qkv[2].wait()
    all_q = project(WQ[...])
    queries = [rotated(all_q[:, head * 128:head * 128 + 128]) for head in range(HEADS)]
    for half in (0, 1):
        rows = [queries[head][core * 64 + half * 32:core * 64 + half * 32 + 32, :] for head in range(HEADS) for core in (0, 1)]
        QT[x, :, half * (COLS // 2):(half + 1) * (COLS // 2)] = jnp.concatenate(rows, axis=0).T
    first_sends((2,))
    for dx in (2, 1, 3):
        q_copy(dx, x).start()
    for cp in load_in(tiles - 1):
        cp.start()

    ACC[:, 128:136, :] = jnp.where(lax.broadcasted_iota(jnp.int32, (4, 8, COLS), 1) == 0, NEG, 0.0)
    ACC[:, 0:128, :] = jnp.zeros((4, 128, COLS), jnp.float32)
    row = lax.broadcasted_iota(jnp.int32, (GROUP, 128), 0)
    run = 2 * (4 * (row // 64) + x) + (row % 64) // 32
    for i in range(MASKED):
        slot_id = (4 * (plain_nb + 2 * i + row // (2 * SLOTS)) + x) * (2 * SLOTS) + row % (2 * SLOTS)
        KPOS[i] = jnp.where(slot_id < cache_len, -1, 1 << 30)
    KPOS[MASKED] = run * 32 + row % 32
    KPOS[MASKED + 1] = (255 - run) * 32 + row % 32

    def units(group, chip, masked):
        cols = [pl.ds(tile * 256, 256) for tile in range(3)]
        key, val_t = KC[group], VC[group]

        def score(i):
            s = jnp.dot(key, QT[chip, :, cols[i]], preferred_element_type=jnp.float32)
            if masked:
                col = lax.broadcasted_iota(jnp.int32, (1, 256), 1) + i * 256
                late = col // (COLS // 2)
                q_run = 2 * (4 * g + chip) + (col % 64) // 32
                q_pos = (q_run + late * (255 - 2 * q_run)) * 32 + col % 32
                k_pos = KPOS[group - plain_nb // 2]
                seen = [k_pos <= q_pos[:, :128], k_pos <= q_pos[:, 128:]]
                s = jnp.concatenate([jnp.where(seen[j], s[:, j * 128:j * 128 + 128], NEG) for j in (0, 1)], axis=1)
            return s

        scores = [score(0)] + [None] * 2
        probs = [None] * 3
        alphas = [None] * 3
        for i in range(4):
            if i < 2:
                scores[i + 1] = score(i + 1)
            if i < 3:
                col, s = cols[i], scores[i]
                old_max = ACC[chip, 128:129, col]
                new_max = jnp.maximum(old_max, jnp.max(s, axis=0, keepdims=True))
                e = jnp.exp2(s * EXP_C - new_max * EXP_C)
                alphas[i] = jnp.exp2((old_max - new_max) * EXP_C)
                ACC[chip, 128:129, col] = new_max
                ACC[chip, 129:130, col] = ACC[chip, 129:130, col] * alphas[i] + jnp.sum(e, axis=0, keepdims=True)
                probs[i] = e.astype(jnp.bfloat16)
            if i > 0:
                col = cols[i - 1]
                ACC[chip, 0:128, col] = ACC[chip, 0:128, col] * alphas[i - 1] + jnp.dot(
                    val_t, probs[i - 1], preferred_element_type=jnp.float32)

    def o_copy(dx):
        dst_x = (x + dx) % 4
        return remote(ACC.at[dst_x], PART.at[dx - 1], o_send.at[dx - 1], o_recv.at[dx - 1], dev(t, g * 4 + dst_x))

    groups = plain_nb // 2

    def step(s, carry):
        count, early, counts = carry[0], carry[1], carry[2:]
        slots, new_count = arrivals(g, s, count)
        next_slots, new_counts = [], []
        for b in range(4):
            nxt, cnt = arrivals(nbr[b], s + 1, counts[b])
            next_slots.append(nxt[b])
            new_counts.append(cnt)
        ring = s <= 8

        def pass_on(b, kind, place):
            last = 8 - b % 2

            @pl.when(s <= last)
            def _():
                ring_copy(b, kind, s, place, zero_slots, zero_slots).wait_recv()

            @pl.when(s < last)
            def _():
                ring_copy(b, kind, s + 1, place, slots, next_slots).start()

        @pl.when(ring)
        def _():
            for_blocks(s, (0, 1, 2), pass_on)

        @pl.when(s == WARM)
        def _():
            for dx in (1, 3, 2):
                q_copy(dx, (x + 4 - dx) % 4).wait_recv()

        phase = s - 9
        dx = jnp.where(phase == 0, 2, jnp.where(phase == 1, 1, jnp.where(phase == 2, 3, 0)))

        @pl.when(s == 9)
        def _():
            for part in (0, 1):
                KC[groups + MASKED + part] = KVN[:, :, 0, part].reshape(GROUP, 128)
                VC[groups + MASKED + part] = KVN[:, :, 1, part].reshape(GROUP, 128).T

        @pl.when(s == 10)
        def _():
            o_copy(2).start()

        @pl.when(s == 11)
        def _():
            o_copy(1).start()

        @pl.when(s == 12)
        def _():
            o_copy(3).start()

        new_early = jnp.where(s < WARM, 0, jnp.where(s < 8, new_count // 4, early))
        first = jnp.where(ring, 4 * early, 0)
        last = jnp.where(ring, 4 * new_early, groups - early)

        def plain(n, inner):
            units(jnp.where(ring, n // 4, early + n), jnp.where(ring, n % 4, (x + dx) % 4), False)
            return inner
        lax.fori_loop(first, last, plain, 0)

        def masked(n, inner):
            units(groups + n, (x + dx) % 4, True)
            return inner
        lax.fori_loop(0, jnp.where(ring, 0, MASKED + 2), masked, 0)
        return (jnp.where(ring, new_count, count), new_early, *new_counts)

    lax.fori_loop(1, 13, step, (own_count + jnp.int32(0), jnp.int32(0), *nbr_counts))

    for dx in (1, 3, 2):
        o_copy(dx).wait_recv()
    maxes = [ACC[x, 128:129, :]] + [PART[i, 128:129, :] for i in range(3)]
    sums = [ACC[x, 129:130, :]] + [PART[i, 129:130, :] for i in range(3)]
    top = functools.reduce(jnp.maximum, maxes)
    weights = [jnp.exp2((m - top) * EXP_C) for m in maxes]
    total = sum(w * l for w, l in zip(weights, sums))
    acc = ACC[x, 0:128, :] * weights[0]
    for i in range(3):
        acc = acc + PART[i, 0:128, :] * weights[i + 1]
    o_rows = (acc / total).T.astype(jnp.bfloat16)
    heads = []
    for head in range(HEADS):
        pieces = []
        for core in (0, 1):
            for half in (0, 1):
                base = half * (COLS // 2) + head * 64 + core * 32
                pieces.append(o_rows[base:base + 32, :])
        heads.append(jnp.concatenate(pieces, axis=0))

    def add_over_cores(i):
        copy = remote(SUM.at[their_rows], GOT.at[i], x_send.at[2 + i], x_recv.at[2 + i], dev(1 - t, c))
        copy.start()
        copy.wait()
        return SUM[my_rows, :] + GOT[i]

    load_out.wait()
    share_norm(0).wait_send()
    SUM[...] = jnp.dot(jnp.concatenate(heads, axis=1), WO[...], preferred_element_type=jnp.float32)
    mid = (hid_ref[...].astype(jnp.float32) + add_over_cores(0)).astype(jnp.bfloat16).astype(jnp.float32)
    normed(1, mid)
    share_norm(1).start()
    norm_landed(1).wait_recv()
    share_norm(1).wait_send()

    def widen(i, carry):
        for cp in load_in(i):
            cp.wait()
        gate = jnp.dot(NORM[1], WG[i], preferred_element_type=jnp.float32)
        up = jnp.dot(NORM[1], WU[i], preferred_element_type=jnp.float32)
        HM[i] = (gate * jax.nn.sigmoid(gate) * up).astype(jnp.bfloat16)
        return carry

    lax.fori_loop(0, tiles, widen, 0)
    SUM[...] = jnp.zeros_like(SUM)

    def narrow(i, carry):
        load_down(i).wait()
        SUM[...] += jnp.dot(HM[i], WD[i], preferred_element_type=jnp.float32)
        return carry

    lax.fori_loop(0, tiles, narrow, 0)
    out_ref[...] = (mid + add_over_cores(1)).astype(jnp.bfloat16)

    for dx in (1, 2, 3):
        q_copy(dx, x).wait_send()
        o_copy(dx).wait_send()

    @pl.when(g < nb)
    def _():
        for cp in sib_copies(t):
            cp.wait_send()

    def drain(s, carry):
        def sent(b, kind, place):
            @pl.when(s < 8 - b % 2)
            def _():
                ring_copy(b, kind, s + 1, place, zero_slots, zero_slots).wait_send()

        for_blocks(s, (0, 1, 2), sent)
        return carry
    lax.fori_loop(0, 8, drain, 0)


def layer(index, cache_len, table, hidden, gains, cache_k, cache_v, w_query, w_key, w_value, w_out, w_gate, w_up, w_down):
    nb = (index + 1) * 16 // BUCKETS
    bf16, f32 = jnp.bfloat16, jnp.float32
    width, ffn = w_gate.shape
    tiles = ffn // FFN_TILE
    vmem = pl.BlockSpec(memory_space=pltpu.VMEM)
    hbm = pl.BlockSpec(memory_space=pl.ANY)
    dma = pltpu.SemaphoreType.DMA
    return pl.pallas_call(
        functools.partial(layer_kernel, nb),
        out_shape=jax.ShapeDtypeStruct(hidden.shape, bf16),
        in_specs=[pl.BlockSpec(memory_space=pltpu.SMEM)] + [vmem] * 5 + [hbm] * 7,
        out_specs=vmem,
        scratch_shapes=[
            pltpu.VMEM((4, 128, COLS), bf16),
            pltpu.VMEM((nb // 2 + 2, GROUP, 128), bf16),
            pltpu.VMEM((nb // 2 + 2, 128, GROUP), bf16),
            pltpu.VMEM((16, 2, 2, 2, 32, 128), bf16),
            pltpu.VMEM((4, 136, COLS), f32),
            pltpu.VMEM((3, 136, COLS), f32),
            pltpu.VMEM((256, SLOTS), bf16),
            pltpu.VMEM((MASKED + 2, GROUP, 128), jnp.int32),
            pltpu.VMEM(w_out.shape, bf16),
            pltpu.VMEM((tiles, width, FFN_TILE), bf16),
            pltpu.VMEM((tiles, width, FFN_TILE), bf16),
            pltpu.VMEM((tiles, FFN_TILE, width), bf16),
            pltpu.VMEM((2, 128, width), bf16),
            pltpu.VMEM((128, width), f32),
            pltpu.VMEM((2, 64, width), f32),
            pltpu.VMEM((tiles, 128, FFN_TILE), bf16),
            dma((4, 3, 9)), dma((4, 3, 9)), dma((3,)), dma((3,)), dma((3,)), dma((3,)), dma((2,)), dma((2,)), dma((2,)),
            dma((4, max(tiles, 4))), dma((4,)), dma((4,)),
        ],
        compiler_params=pltpu.CompilerParams(collective_id=index, has_side_effects=True, vmem_limit_bytes=67043328),
        name='layer_%d' % nb,
    )(cache_len, table, hidden, gains, cache_k, cache_v, w_query, w_key, w_value, w_out, w_gate, w_up, w_down)


def solution(mesh):
    token_spec = P(('dp', 'cp', 'tp'), None)
    column_spec = P(None, 'tp')
    row_spec = P('tp', None)

    def device_layer(hidden_loc, pos_loc, cache_len, cache_k, cache_v, norm1_gain, w_query, w_key, w_value, w_out, norm2_gain, w_gate, w_up, w_down):
        row = jnp.arange(128, dtype=jnp.int32)
        run = 2 * lax.axis_index('cp') + row // 64
        run = jnp.where(row % 64 < 32, run, 255 - run)
        table = rotary_table(cache_len[0] + run * 32 + row % 32)
        gains = jnp.stack([norm1_gain, norm2_gain])
        bucket = jnp.clip((cache_len[0] - 1) // (128 * SLOTS // BUCKETS), 0, BUCKETS - 1)
        return lax.switch(bucket, [functools.partial(layer, i) for i in range(BUCKETS)], cache_len, table, hidden_loc, gains,
                          cache_k, cache_v, w_query, w_key, w_value, w_out, w_gate, w_up, w_down)

    return jax.shard_map(device_layer, mesh=mesh, in_specs=(token_spec, P(('dp', 'cp', 'tp')), P('dp'), token_spec, token_spec, P(), column_spec, column_spec, column_spec, row_spec, P(), column_spec, column_spec, row_spec), out_specs=token_spec, check_vma=False)
```

```python
import functools
import math
import jax
import jax.numpy as jnp
from jax import lax
from jax.experimental import pallas as pl
from jax.experimental.pallas import tpu as pltpu
from jax.sharding import PartitionSpec as P

HEAD_DIM = 128
ROPE_BASE = 500000.0
NORM_EPS = 1e-5
HEADS = 6
SLOTS = 256
COLS = HEADS * 128
GROUP = 8 * SLOTS
FFN_TILE = 896
TILE = 256
HELD = 3
NEG = -2.3e38
EXP_C = math.log2(math.e) / math.sqrt(HEAD_DIM)
BUCKETS = 4


def rotary_table(positions):
    half_dim = HEAD_DIM // 2
    inv_freq = 1.0 / (ROPE_BASE ** (jnp.arange(half_dim, dtype=jnp.float32) * (2.0 / HEAD_DIM)))
    angles = positions.astype(jnp.float32)[:, None] * inv_freq[None, :]
    cos_table, sin_table = jnp.cos(angles), jnp.sin(angles)
    return jnp.stack([jnp.concatenate([cos_table, cos_table], axis=1), jnp.concatenate([-sin_table, sin_table], axis=1)])


def layer_kernel(nb, len_ref, table_ref, hid_ref, gain_ref, ck_ref, cv_ref,
                 wq_hbm, wk_hbm, wv_hbm, wo_hbm, wg_hbm, wu_hbm, wd_hbm, out_ref,
                 QT, KC, VC, KVN, ACC, PART, VTS, KPOS, WO, WG, WU, WD, NORM, SUM, GOT, HM,
                 send_sem, recv_sem, q_send, q_recv, o_send, o_recv, sib_send, sib_recv, loc_sem, w_sem, x_send, x_recv):
    c = lax.axis_index('cp')
    t = lax.axis_index('tp')
    x = c % 4
    g = c // 4
    cache_len = len_ref[0]
    plain_nb = nb - 4

    def dev(core, chip):
        return {'tp': core, 'cp': chip}

    z, y = g // 4, g % 4

    def place_at(h, a, b):
        c1 = lax.rem(y * (1 - h) + z * h + a + 4, 4)
        c2 = lax.rem(z * (1 - h) + y * h + b + 4, 4)
        return (4 * c2 + c1) * (1 - h) + (4 * c1 + c2) * h

    def offset(i):
        return jnp.where(i == 3, 2, jnp.where(i == 0, 0, 2 * i - 3))

    barrier = pltpu.get_barrier_semaphore()
    partners = [dev(t, place_at(0, a, b) * 4 + x) for a, b in ((-1, 0), (1, 0), (0, -1), (0, 1))]
    partners += [dev(t, g * 4 + (x + dx) % 4) for dx in (1, 2, 3)] + [dev(1 - t, c)]
    for p in partners:
        pl.semaphore_signal(barrier, inc=1, device_id=p, device_id_type=pl.DeviceIdType.MESH)

    tiles = HM.shape[0]
    held = WG.shape[0]

    def load_in(i):
        cols = pl.ds(pl.multiple_of(i * FFN_TILE, HEAD_DIM), FFN_TILE)
        return (pltpu.make_async_copy(wg_hbm.at[:, cols], WG.at[lax.rem(i, held)], w_sem.at[1, i]),
                pltpu.make_async_copy(wu_hbm.at[:, cols], WU.at[lax.rem(i, held)], w_sem.at[2, i]))

    def load_down(i):
        return pltpu.make_async_copy(wd_hbm.at[pl.ds(i * FFN_TILE, FFN_TILE), :], WD.at[lax.rem(i, WD.shape[0])], w_sem.at[3, i])

    WQ = WG.at[held - 1, :, 0:HEADS * HEAD_DIM]
    WK, WV = WU.at[held - 1, :, 0:HEAD_DIM], WU.at[held - 1, :, HEAD_DIM:TILE]
    load_qkv = [pltpu.make_async_copy(wk_hbm, WK, w_sem.at[0, 0]), pltpu.make_async_copy(wv_hbm, WV, w_sem.at[0, 1]),
                pltpu.make_async_copy(wq_hbm, WQ, w_sem.at[0, 2])]
    load_out = pltpu.make_async_copy(wo_hbm, WO, w_sem.at[0, 3])
    for cp in load_qkv:
        cp.start()
    load_out.start()
    for i in range(held - 1):
        for cp in load_in(i):
            cp.start()
    for i in range(WD.shape[0]):
        load_down(i).start()

    my_rows = pl.ds(pl.multiple_of(t * 64, 64), 64)
    their_rows = pl.ds(pl.multiple_of((1 - t) * 64, 64), 64)

    def normed(i, values):
        inv_rms = lax.rsqrt(jnp.mean(values * values, axis=-1, keepdims=True) + NORM_EPS)
        NORM[i, my_rows, :] = (values * inv_rms * gain_ref[i:i + 1, :].astype(jnp.float32)).astype(jnp.bfloat16)

    VTS[...] = cv_ref[...].T
    normed(0, hid_ref[...].astype(jnp.float32))
    ACC[:, HEAD_DIM:136, :] = jnp.where(lax.broadcasted_iota(jnp.int32, (4, 8, COLS), 1) == 0, NEG, 0.0)
    ACC[:, 0:HEAD_DIM, :] = jnp.zeros((4, HEAD_DIM, COLS), jnp.float32)
    row = lax.broadcasted_iota(jnp.int32, (GROUP, HEAD_DIM), 0)
    slot_id = (4 * (plain_nb + row // (2 * SLOTS)) + x) * (2 * SLOTS) + row % (2 * SLOTS)
    KPOS[0] = jnp.where(slot_id < cache_len, -1, 1 << 30)
    run = 2 * (4 * (row % (GROUP // 2) // 64) + x) + (row % 64) // 32
    KPOS[1] = jnp.where(row < GROUP // 2, run, 255 - run) * 32 + row % 32
    pl.semaphore_wait(barrier, len(partners))

    def remote(src, dst, send, recv, device):
        return pltpu.make_async_remote_copy(src_ref=src, dst_ref=dst, send_sem=send, recv_sem=recv,
                                            device_id=device, device_id_type=pl.DeviceIdType.MESH)

    def q_copy(dx, chip_x):
        return remote(QT.at[x], QT.at[chip_x], q_send.at[dx - 1], q_recv.at[dx - 1], dev(t, g * 4 + (x + dx) % 4))

    def slot_of(kind, place, h):
        if kind == 2:
            return KVN.at[place, h]
        span = pl.ds(pl.multiple_of((lax.rem(place, 4) * 2 + h) * SLOTS, SLOTS), SLOTS)
        return KC.at[lax.div(place, 4), span, :] if kind == 0 else VC.at[lax.div(place, 4), :, span]

    mine = pl.ds(pl.multiple_of(t * HEAD_DIM, HEAD_DIM), HEAD_DIM)
    other = pl.ds(pl.multiple_of((1 - t) * HEAD_DIM, HEAD_DIM), HEAD_DIM)

    def sib_copies(h):
        return (remote(ck_ref.at[:, other], slot_of(0, g, h), sib_send.at[0], sib_recv.at[0], dev(1 - t, c)),
                remote(VTS.at[other], slot_of(1, g, h), sib_send.at[1], sib_recv.at[1], dev(1 - t, c)))

    local_cache = [pltpu.make_async_copy(ck_ref.at[:, mine], slot_of(0, g, t), loc_sem.at[0]),
                   pltpu.make_async_copy(VTS.at[mine], slot_of(1, g, t), loc_sem.at[1])]

    def share_norm(i):
        rows = NORM.at[i, my_rows]
        return remote(rows, rows, x_send.at[i], x_recv.at[i], dev(1 - t, c))

    def norm_landed(i):
        rows = NORM.at[i, their_rows]
        return remote(rows, rows, x_send.at[i], x_recv.at[i], dev(1 - t, c))

    share_norm(0).start()

    @pl.when(g < nb)
    def _():
        for cp in sib_copies(t):
            cp.start()
        for cp in local_cache:
            cp.start()

    def piece(kind, h, block, target, seen):
        place = place_at(h, *block)
        index = lax.rem(seen[0] + 4, 4) * 4 + lax.rem(seen[1] + 4, 4)
        ref = slot_of(kind, place, h)
        return remote(ref, ref, send_sem.at[h, kind, index], recv_sem.at[h, kind, index], dev(t, place_at(h, *target) * 4 + x))

    def when_live(kind, h, block, fn):
        if kind < 2:
            pl.when(place_at(h, *block) < nb)(fn)
        else:
            fn()

    def forward(kind, h):
        return (1, -1, 1 - 2 * h)[kind]

    def spread(kind, h, a):
        for sign in (1, -1):
            piece(kind, h, (a, 0), (0, sign), (a, -sign)).start()

    def own_sends(kinds):
        def body(h, carry):
            for kind in kinds:
                def go():
                    for sign in (1, -1):
                        piece(kind, h, (0, 0), (sign, 0), (-sign, 0)).start()
                    spread(kind, h, 0)
                when_live(kind, h, (0, 0), go)
            return carry
        lax.fori_loop(0, 2, body, 0)

    @pl.when(g < nb)
    def _():
        for cp in local_cache:
            cp.wait()
        for cp in sib_copies(1 - t):
            cp.wait_recv()

    own_sends((0, 1))

    norm_landed(0).wait_recv()

    def project(weight):
        return jnp.dot(NORM[0], weight, preferred_element_type=jnp.float32)

    def rotated(head):
        return (head * table_ref[0] + pltpu.roll(head, 64, 1) * table_ref[1]).astype(jnp.bfloat16)

    for cp in load_qkv[:2]:
        cp.wait()
    new_kv = (rotated(project(WK[...])), project(WV[...]).astype(jnp.bfloat16))
    for kv in (0, 1):
        for core in (0, 1):
            for half in (0, 1):
                base = core * 64 + half * 32
                KVN[g, core, kv, half] = new_kv[kv][base:base + 32, :]
    load_qkv[2].wait()

    def project_pair(i, carry):
        both = project(WG[held - 1, :, pl.ds(pl.multiple_of(i * TILE, TILE), TILE)])
        pair = [rotated(both[:, :HEAD_DIM]), rotated(both[:, HEAD_DIM:])]
        for half in (0, 1):
            rows = [head[core * 64 + half * 32:core * 64 + half * 32 + 32, :] for head in pair for core in (0, 1)]
            QT[x, :, pl.ds(pl.multiple_of(half * (COLS // 2) + i * HEAD_DIM, HEAD_DIM), HEAD_DIM)] = jnp.concatenate(rows, axis=0).T
        return carry

    lax.fori_loop(0, HEADS // 2, project_pair, 0)
    own_sends((2,))
    for dx in (2, 1, 3):
        q_copy(dx, x).start()
    for cp in load_in(held - 1):
        cp.start()

    def units(group, chip, masked):
        cols = [pl.ds(tile * TILE, TILE) for tile in range(3)]
        key, val_t = KC[group], VC[group]

        def score(i):
            s = jnp.dot(key, QT[chip, :, cols[i]], preferred_element_type=jnp.float32)
            if masked:
                col = lax.broadcasted_iota(jnp.int32, (1, TILE), 1) + i * TILE
                late = col // (COLS // 2)
                q_run = 2 * (4 * g + chip) + (col % 64) // 32
                q_pos = (q_run + late * (255 - 2 * q_run)) * 32 + col % 32
                k_pos = KPOS[group - plain_nb // 4]
                seen = [k_pos <= q_pos[:, :HEAD_DIM], k_pos <= q_pos[:, HEAD_DIM:]]
                s = jnp.concatenate([jnp.where(seen[j], s[:, j * HEAD_DIM:j * HEAD_DIM + HEAD_DIM], NEG) for j in (0, 1)], axis=1)
            return s

        scores = [score(0)] + [None] * 2
        probs = [None] * 3
        alphas = [None] * 3
        for i in range(4):
            if i < 2:
                scores[i + 1] = score(i + 1)
            if i < 3:
                col, s = cols[i], scores[i]
                old_max = ACC[chip, HEAD_DIM:129, col]
                new_max = jnp.maximum(old_max, jnp.max(s, axis=0, keepdims=True))
                e = jnp.exp2(s * EXP_C - new_max * EXP_C)
                alphas[i] = jnp.exp2((old_max - new_max) * EXP_C)
                ACC[chip, HEAD_DIM:129, col] = new_max
                ACC[chip, 129:130, col] = ACC[chip, 129:130, col] * alphas[i] + jnp.sum(e, axis=0, keepdims=True)
                probs[i] = e.astype(jnp.bfloat16)
            if i > 0:
                col = cols[i - 1]
                ACC[chip, 0:HEAD_DIM, col] = ACC[chip, 0:HEAD_DIM, col] * alphas[i - 1] + jnp.dot(
                    val_t, probs[i - 1], preferred_element_type=jnp.float32)

    def o_copy(dx):
        dst_x = (x + dx) % 4
        return remote(ACC.at[dst_x], PART.at[dx - 1], o_send.at[dx - 1], o_recv.at[dx - 1], dev(t, g * 4 + dst_x))

    def near(i, carry):
        h = lax.div(i, 2)
        a = 2 * lax.rem(i, 2) - 1
        for kind in range(3):
            def go():
                piece(kind, h, (a, 0), (a, 0), (a, 0)).wait_recv()

                @pl.when(a == -forward(kind, h))
                def _():
                    piece(kind, h, (a, 0), (-a, 0), (2, 0)).start()

                spread(kind, h, a)
            when_live(kind, h, (a, 0), go)
        return carry

    lax.fori_loop(0, 4, near, 0)

    def far(h, carry):
        for kind in range(3):
            def go():
                piece(kind, h, (2, 0), (1, 0), (2, 0)).wait_recv()
                spread(kind, h, 2)
            when_live(kind, h, (2, 0), go)
        return carry

    def lines(i, carry):
        @pl.when(i == 4)
        def _():
            lax.fori_loop(0, 2, far, 0)
        a = offset(lax.div(i, 4))
        h = lax.rem(lax.div(i, 2), 2)
        b = 2 * lax.rem(i, 2) - 1
        for kind in range(3):
            def go():
                piece(kind, h, (a, b), (0, b), (a, b)).wait_recv()

                @pl.when(b == -forward(kind, h))
                def _():
                    piece(kind, h, (a, b), (0, -b), (a, 2)).start()
            when_live(kind, h, (a, b), go)
        return carry

    lax.fori_loop(0, 16, lines, 0)

    def far_lines(i, carry):
        a = offset(lax.div(i, 2))
        h = lax.rem(i, 2)
        for kind in range(3):
            def go():
                piece(kind, h, (a, 2), (0, 1), (a, 2)).wait_recv()
            when_live(kind, h, (a, 2), go)
        return carry

    lax.fori_loop(0, 8, far_lines, 0)

    groups = plain_nb // 4
    for part in (0, 1):
        span = slice(part * GROUP // 2, (part + 1) * GROUP // 2)
        KC[groups + 1, span, :] = KVN[:, :, 0, part].reshape(GROUP // 2, HEAD_DIM)
        VC[groups + 1, :, span] = KVN[:, :, 1, part].reshape(GROUP // 2, HEAD_DIM).T
    for dx in (1, 3, 2):
        q_copy(dx, (x + 4 - dx) % 4).wait_recv()

    def chip_phase(phase, carry):
        for order, dx in ((1, 2), (2, 1), (3, 3)):
            @pl.when(phase == order)
            def _():
                o_copy(dx).start()
        dx = jnp.where(phase == 0, 2, jnp.where(phase == 1, 1, jnp.where(phase == 2, 3, 0)))
        chip = (x + dx) % 4

        def plain(n, inner):
            units(n, chip, False)
            return inner
        lax.fori_loop(0, groups, plain, 0)

        def masked(n, inner):
            units(groups + n, chip, True)
            return inner
        lax.fori_loop(0, 2, masked, 0)
        return carry

    lax.fori_loop(0, 4, chip_phase, 0)

    for dx in (1, 2, 3):
        q_copy(dx, x).wait_send()

    @pl.when(g < nb)
    def _():
        for cp in sib_copies(t):
            cp.wait_send()

    def drain(i, carry):
        h = lax.rem(i, 2)
        a, b = offset(lax.div(i, 8)), offset(lax.rem(lax.div(i, 2), 4))
        for kind in range(3):
            up = -forward(kind, h)
            first = jnp.where(b == 0, jnp.where(a == 2, up, 0), a)
            second = jnp.where(b == 2, up, 0)

            def go():
                piece(kind, h, (first, second), (1, 0), (a, b)).wait_send()

            def sent():
                when_live(kind, h, (first, second), go)
            pl.when(i >= 2)(sent)
        return carry

    lax.fori_loop(0, 32, drain, 0)

    for dx in (1, 3, 2):
        o_copy(dx).wait()
    maxes = [ACC[x, HEAD_DIM:129, :]] + [PART[i, HEAD_DIM:129, :] for i in range(3)]
    sums = [ACC[x, 129:130, :]] + [PART[i, 129:130, :] for i in range(3)]
    top = functools.reduce(jnp.maximum, maxes)
    weights = [jnp.exp2((m - top) * EXP_C) for m in maxes]
    total = sum(w * l for w, l in zip(weights, sums))
    acc = ACC[x, 0:HEAD_DIM, :] * weights[0]
    for i in range(3):
        acc = acc + PART[i, 0:HEAD_DIM, :] * weights[i + 1]
    o_rows = (acc / total).T.astype(jnp.bfloat16)
    heads = []
    for head in range(HEADS):
        pieces = []
        for core in (0, 1):
            for half in (0, 1):
                base = half * (COLS // 2) + head * 64 + core * 32
                pieces.append(o_rows[base:base + 32, :])
        heads.append(jnp.concatenate(pieces, axis=0))

    def add_over_cores(i):
        copy = remote(SUM.at[their_rows], GOT.at[i], x_send.at[2 + i], x_recv.at[2 + i], dev(1 - t, c))
        copy.start()
        copy.wait()
        return SUM[my_rows, :] + GOT[i]

    load_out.wait()
    share_norm(0).wait_send()
    NORM[0, :, 0:HEADS * HEAD_DIM] = jnp.concatenate(heads, axis=1)

    def project_out(i, carry):
        cols = pl.ds(pl.multiple_of(i * 512, 512), 512)
        SUM[:, cols] = jnp.dot(NORM[0, :, 0:HEADS * HEAD_DIM], WO[:, cols], preferred_element_type=jnp.float32)
        return carry

    lax.fori_loop(0, SUM.shape[1] // 512, project_out, 0)
    mid = (hid_ref[...].astype(jnp.float32) + add_over_cores(0)).astype(jnp.bfloat16).astype(jnp.float32)
    normed(1, mid)
    share_norm(1).start()
    norm_landed(1).wait_recv()
    share_norm(1).wait_send()

    def widen(i, carry):
        for cp in load_in(i):
            cp.wait()
        gate = jnp.dot(NORM[1], WG[lax.rem(i, held)], preferred_element_type=jnp.float32)
        up = jnp.dot(NORM[1], WU[lax.rem(i, held)], preferred_element_type=jnp.float32)
        HM[i] = (gate * jax.nn.sigmoid(gate) * up).astype(jnp.bfloat16)

        @pl.when(i + held < tiles)
        def _():
            for cp in load_in(i + held):
                cp.start()
        return carry

    lax.fori_loop(0, tiles, widen, 0)
    SUM[...] = jnp.zeros_like(SUM)

    def narrow(i, carry):
        load_down(i).wait()
        SUM[...] += jnp.dot(HM[i], WD[lax.rem(i, WD.shape[0])], preferred_element_type=jnp.float32)

        @pl.when(i + WD.shape[0] < tiles)
        def _():
            load_down(i + WD.shape[0]).start()
        return carry

    lax.fori_loop(0, tiles, narrow, 0)
    out_ref[...] = (mid + add_over_cores(1)).astype(jnp.bfloat16)


def layer(index, cache_len, table, hidden, gains, cache_k, cache_v, w_query, w_key, w_value, w_out, w_gate, w_up, w_down):
    nb = (index + 1) * 16 // BUCKETS
    bf16, f32 = jnp.bfloat16, jnp.float32
    width, ffn = w_gate.shape
    tiles = ffn // FFN_TILE
    vmem = pl.BlockSpec(memory_space=pltpu.VMEM)
    hbm = pl.BlockSpec(memory_space=pl.ANY)
    dma = pltpu.SemaphoreType.DMA
    return pl.pallas_call(
        functools.partial(layer_kernel, nb),
        out_shape=jax.ShapeDtypeStruct(hidden.shape, bf16),
        in_specs=[pl.BlockSpec(memory_space=pltpu.SMEM)] + [vmem] * 5 + [hbm] * 7,
        out_specs=vmem,
        scratch_shapes=[
            pltpu.VMEM((4, HEAD_DIM, COLS), bf16),
            pltpu.VMEM((nb // 4 + 1, GROUP, HEAD_DIM), bf16),
            pltpu.VMEM((nb // 4 + 1, HEAD_DIM, GROUP), bf16),
            pltpu.VMEM((16, 2, 2, 2, 32, HEAD_DIM), bf16),
            pltpu.VMEM((4, 136, COLS), f32),
            pltpu.VMEM((3, 136, COLS), f32),
            pltpu.VMEM((TILE, SLOTS), bf16),
            pltpu.VMEM((2, GROUP, HEAD_DIM), jnp.int32),
            pltpu.VMEM(w_out.shape, bf16),
            pltpu.VMEM((HELD, width, FFN_TILE), bf16),
            pltpu.VMEM((HELD, width, FFN_TILE), bf16),
            pltpu.VMEM((HELD + 1, FFN_TILE, width), bf16),
            pltpu.VMEM((2, HEAD_DIM, width), bf16),
            pltpu.VMEM((HEAD_DIM, width), f32),
            pltpu.VMEM((2, 64, width), f32),
            pltpu.VMEM((tiles, HEAD_DIM, FFN_TILE), bf16),
            dma((2, 3, 16)), dma((2, 3, 16)), dma((3,)), dma((3,)), dma((3,)), dma((3,)), dma((2,)), dma((2,)), dma((2,)),
            dma((4, max(tiles, 4))), dma((4,)), dma((4,)),
        ],
        compiler_params=pltpu.CompilerParams(collective_id=index, has_side_effects=True, vmem_limit_bytes=67043328),
        name='layer_%d' % nb,
    )(cache_len, table, hidden, gains, cache_k, cache_v, w_query, w_key, w_value, w_out, w_gate, w_up, w_down)


def solution(mesh):
    token_spec = P(('dp', 'cp', 'tp'), None)
    column_spec = P(None, 'tp')
    row_spec = P('tp', None)

    def device_layer(hidden_loc, pos_loc, cache_len, cache_k, cache_v, norm1_gain, w_query, w_key, w_value, w_out, norm2_gain, w_gate, w_up, w_down):
        row = jnp.arange(HEAD_DIM, dtype=jnp.int32)
        run = 2 * lax.axis_index('cp') + row // 64
        run = jnp.where(row % 64 < 32, run, 255 - run)
        table = rotary_table(cache_len[0] + run * 32 + row % 32)
        gains = jnp.stack([norm1_gain, norm2_gain])
        bucket = jnp.clip((cache_len[0] - 1) // (HEAD_DIM * SLOTS // BUCKETS), 0, BUCKETS - 1)
        return lax.switch(bucket, [functools.partial(layer, i) for i in range(BUCKETS)], cache_len, table, hidden_loc, gains,
                          cache_k, cache_v, w_query, w_key, w_value, w_out, w_gate, w_up, w_down)

    return jax.shard_map(device_layer, mesh=mesh, in_specs=(token_spec, P(('dp', 'cp', 'tp')), P('dp'), token_spec, token_spec, P(), column_spec, column_spec, column_spec, row_spec, P(), column_spec, column_spec, row_spec), out_specs=token_spec, check_vma=False)
```

```python
import functools
import math
import jax
import jax.numpy as jnp
from jax import lax
from jax.experimental import pallas as pl
from jax.experimental.pallas import tpu as pltpu
from jax.sharding import PartitionSpec as P

HEAD_DIM = 128
ROPE_BASE = 500000.0
NORM_EPS = 1e-5
HEADS = 6
SLOTS = 256
COLS = HEADS * 128
GROUP = 8 * SLOTS
FFN_TILE = 896
O_ROWS, M_ROW, L_ROW = slice(0, HEAD_DIM), slice(HEAD_DIM, HEAD_DIM + 1), slice(HEAD_DIM + 1, HEAD_DIM + 2)
TILE = 256
HELD = 3
NEG = -2.3e38
EXP_C = math.log2(math.e) / math.sqrt(HEAD_DIM)
BUCKETS = (8, 12, 16)


def rotary_table(positions):
    half_dim = HEAD_DIM // 2
    inv_freq = 1.0 / (ROPE_BASE ** (jnp.arange(half_dim, dtype=jnp.float32) * (2.0 / HEAD_DIM)))
    angles = positions.astype(jnp.float32)[:, None] * inv_freq[None, :]
    cos_table, sin_table = jnp.cos(angles), jnp.sin(angles)
    return jnp.stack([jnp.concatenate([cos_table, cos_table], axis=1), jnp.concatenate([-sin_table, sin_table], axis=1)])


def layer_kernel(nb, plain_nb, len_ref, table_ref, hid_ref, gain_ref, ck_ref, cv_ref,
                 wq_hbm, wk_hbm, wv_hbm, wo_hbm, wg_hbm, wu_hbm, wd_hbm, out_ref,
                 QT, KC, VC, KVN, ACC, PART, VTS, KPOS, WO, WG, WU, WD, NORM, SUM, GOT, HM,
                 send_sem, recv_sem, q_send, q_recv, o_send, o_recv, sib_send, sib_recv, loc_sem, w_sem, x_send, x_recv):
    c = lax.axis_index('cp')
    t = lax.axis_index('tp')
    x = c % 4
    g = c // 4
    cache_len = len_ref[0]
    cache_masked = (nb - plain_nb) // 4

    def dev(core, chip):
        return {'tp': core, 'cp': chip}

    z, y = g // 4, g % 4

    def place_at(h, a, b):
        c1 = lax.rem(y * (1 - h) + z * h + a + 4, 4)
        c2 = lax.rem(z * (1 - h) + y * h + b + 4, 4)
        return (4 * c2 + c1) * (1 - h) + (4 * c1 + c2) * h

    def offset(i):
        return jnp.where(i == 3, 2, jnp.where(i == 0, 0, 2 * i - 3))

    barrier = pltpu.get_barrier_semaphore()
    partners = [dev(t, place_at(0, a, b) * 4 + x) for a, b in ((-1, 0), (1, 0), (0, -1), (0, 1))]
    partners += [dev(t, g * 4 + (x + dx) % 4) for dx in (1, 2, 3)] + [dev(1 - t, c)]
    for p in partners:
        pl.semaphore_signal(barrier, inc=1, device_id=p, device_id_type=pl.DeviceIdType.MESH)

    tiles = HM.shape[0]
    held = WG.shape[0]

    def load_in(i):
        cols = pl.ds(pl.multiple_of(i * FFN_TILE, HEAD_DIM), FFN_TILE)
        return (pltpu.make_async_copy(wg_hbm.at[:, cols], WG.at[lax.rem(i, held)], w_sem.at[1, i]),
                pltpu.make_async_copy(wu_hbm.at[:, cols], WU.at[lax.rem(i, held)], w_sem.at[2, i]))

    def load_down(i):
        return pltpu.make_async_copy(wd_hbm.at[pl.ds(i * FFN_TILE, FFN_TILE), :], WD.at[lax.rem(i, WD.shape[0])], w_sem.at[3, i])

    WQ = WG.at[held - 1, :, 0:HEADS * HEAD_DIM]
    WK, WV = WU.at[held - 1, :, 0:HEAD_DIM], WU.at[held - 1, :, HEAD_DIM:TILE]
    load_qkv = [pltpu.make_async_copy(wk_hbm, WK, w_sem.at[0, 0]), pltpu.make_async_copy(wv_hbm, WV, w_sem.at[0, 1]),
                pltpu.make_async_copy(wq_hbm, WQ, w_sem.at[0, 2])]
    load_out = pltpu.make_async_copy(wo_hbm, WO, w_sem.at[0, 3])
    for cp in load_qkv:
        cp.start()
    load_out.start()
    for i in range(held - 1):
        for cp in load_in(i):
            cp.start()
    for i in range(WD.shape[0]):
        load_down(i).start()

    my_rows = pl.ds(pl.multiple_of(t * 64, 64), 64)
    their_rows = pl.ds(pl.multiple_of((1 - t) * 64, 64), 64)

    def normed(i, values):
        inv_rms = lax.rsqrt(jnp.mean(values * values, axis=-1, keepdims=True) + NORM_EPS)
        NORM[i, my_rows, :] = (values * inv_rms * gain_ref[i:i + 1, :].astype(jnp.float32)).astype(jnp.bfloat16)

    VTS[...] = cv_ref[...].T
    normed(0, hid_ref[...].astype(jnp.float32))
    ACC[:, HEAD_DIM:136, :] = jnp.where(lax.broadcasted_iota(jnp.int32, (4, 8, COLS), 1) == 0, NEG, 0.0)
    ACC[:, O_ROWS, :] = jnp.zeros((4, HEAD_DIM, COLS), jnp.float32)
    row = lax.broadcasted_iota(jnp.int32, (GROUP, HEAD_DIM), 0)
    for i in range(cache_masked):
        slot_id = (4 * (plain_nb + 4 * i + row // (2 * SLOTS)) + x) * (2 * SLOTS) + row % (2 * SLOTS)
        KPOS[i] = jnp.where(slot_id < cache_len, -1, 1 << 30)
    run = 2 * (4 * (row % (GROUP // 2) // 64) + x) + (row % 64) // 32
    KPOS[cache_masked] = jnp.where(row < GROUP // 2, run, 255 - run) * 32 + row % 32
    pl.semaphore_wait(barrier, len(partners))

    def remote(src, dst, send, recv, device):
        return pltpu.make_async_remote_copy(src_ref=src, dst_ref=dst, send_sem=send, recv_sem=recv,
                                            device_id=device, device_id_type=pl.DeviceIdType.MESH)

    def q_copy(dx, chip_x):
        return remote(QT.at[x], QT.at[chip_x], q_send.at[dx - 1], q_recv.at[dx - 1], dev(t, g * 4 + (x + dx) % 4))

    def slot_of(kind, place, h):
        if kind == 2:
            return KVN.at[place, h]
        span = pl.ds(pl.multiple_of((lax.rem(place, 4) * 2 + h) * SLOTS, SLOTS), SLOTS)
        return KC.at[lax.div(place, 4), span, :] if kind == 0 else VC.at[lax.div(place, 4), :, span]

    mine = pl.ds(pl.multiple_of(t * HEAD_DIM, HEAD_DIM), HEAD_DIM)
    other = pl.ds(pl.multiple_of((1 - t) * HEAD_DIM, HEAD_DIM), HEAD_DIM)

    def sib_copies(h):
        return (remote(ck_ref.at[:, other], slot_of(0, g, h), sib_send.at[0], sib_recv.at[0], dev(1 - t, c)),
                remote(VTS.at[other], slot_of(1, g, h), sib_send.at[1], sib_recv.at[1], dev(1 - t, c)))

    local_cache = [pltpu.make_async_copy(ck_ref.at[:, mine], slot_of(0, g, t), loc_sem.at[0]),
                   pltpu.make_async_copy(VTS.at[mine], slot_of(1, g, t), loc_sem.at[1])]

    def share_norm(i):
        rows = NORM.at[i, my_rows]
        return remote(rows, rows, x_send.at[i], x_recv.at[i], dev(1 - t, c))

    def norm_landed(i):
        rows = NORM.at[i, their_rows]
        return remote(rows, rows, x_send.at[i], x_recv.at[i], dev(1 - t, c))

    share_norm(0).start()

    @pl.when(g < nb)
    def _():
        for cp in sib_copies(t):
            cp.start()
        for cp in local_cache:
            cp.start()

    def piece(kind, h, block, target, seen):
        place = place_at(h, *block)
        index = lax.rem(seen[0] + 4, 4) * 4 + lax.rem(seen[1] + 4, 4)
        ref = slot_of(kind, place, h)
        return remote(ref, ref, send_sem.at[h, kind, index], recv_sem.at[h, kind, index], dev(t, place_at(h, *target) * 4 + x))

    def when_live(kind, h, block, fn):
        if kind < 2:
            pl.when(place_at(h, *block) < nb)(fn)
        else:
            fn()

    def forward(kind, h):
        return (1, -1, 1 - 2 * h)[kind]

    def way(kind, h, first_axis, step):
        usual = forward(kind, h)
        if kind == 2 or nb != 8:
            return usual
        on_z = h if first_axis else 1 - h
        return jnp.where(on_z == 1, jnp.where(lax.rem(z + step + 4, 4) == 0, -1, 1), usual)

    def spread(kind, h, a):
        for sign in (1, -1):
            piece(kind, h, (a, 0), (0, sign), (a, -sign)).start()

    def own_sends(kinds):
        def body(h, carry):
            for kind in kinds:
                def go():
                    for sign in (1, -1):
                        piece(kind, h, (0, 0), (sign, 0), (-sign, 0)).start()
                    spread(kind, h, 0)
                when_live(kind, h, (0, 0), go)
            return carry
        lax.fori_loop(0, 2, body, 0)

    @pl.when(g < nb)
    def _():
        for cp in local_cache:
            cp.wait()
        for cp in sib_copies(1 - t):
            cp.wait_recv()

    own_sends((0, 1))

    norm_landed(0).wait_recv()

    def project(weight):
        return jnp.dot(NORM[0], weight, preferred_element_type=jnp.float32)

    def rotated(head):
        return (head * table_ref[0] + pltpu.roll(head, 64, 1) * table_ref[1]).astype(jnp.bfloat16)

    for cp in load_qkv[:2]:
        cp.wait()
    new_kv = (rotated(project(WK[...])), project(WV[...]).astype(jnp.bfloat16))
    for kv in (0, 1):
        for core in (0, 1):
            for half in (0, 1):
                base = core * 64 + half * 32
                KVN[g, core, kv, half] = new_kv[kv][base:base + 32, :]
    load_qkv[2].wait()

    def project_pair(i, carry):
        both = project(WG[held - 1, :, pl.ds(pl.multiple_of(i * TILE, TILE), TILE)])
        pair = [rotated(both[:, :HEAD_DIM]), rotated(both[:, HEAD_DIM:])]
        for half in (0, 1):
            rows = [head[core * 64 + half * 32:core * 64 + half * 32 + 32, :] for head in pair for core in (0, 1)]
            QT[x, :, pl.ds(pl.multiple_of(half * (COLS // 2) + i * HEAD_DIM, HEAD_DIM), HEAD_DIM)] = jnp.concatenate(rows, axis=0).T
        return carry

    lax.fori_loop(0, HEADS // 2, project_pair, 0)
    own_sends((2,))
    for dx in (2, 1, 3):
        q_copy(dx, x).start()
    for cp in load_in(held - 1):
        cp.start()

    def units(group, chip, masked):
        cols = [pl.ds(tile * TILE, TILE) for tile in range(3)]
        key, val_t = KC[group], VC[group]

        def score(i):
            s = jnp.dot(key, QT[chip, :, cols[i]], preferred_element_type=jnp.float32)
            if masked:
                col = lax.broadcasted_iota(jnp.int32, (1, TILE), 1) + i * TILE
                late = col // (COLS // 2)
                q_run = 2 * (4 * g + chip) + (col % 64) // 32
                q_pos = (q_run + late * (255 - 2 * q_run)) * 32 + col % 32
                k_pos = KPOS[group - plain_nb // 4]
                seen = [k_pos <= q_pos[:, :HEAD_DIM], k_pos <= q_pos[:, HEAD_DIM:]]
                s = jnp.concatenate([jnp.where(seen[j], s[:, j * HEAD_DIM:j * HEAD_DIM + HEAD_DIM], NEG) for j in (0, 1)], axis=1)
            return s

        scores = [score(0)] + [None] * 2
        probs = [None] * 3
        alphas = [None] * 3
        for i in range(4):
            if i < 2:
                scores[i + 1] = score(i + 1)
            if i < 3:
                col, s = cols[i], scores[i]
                old_max = ACC[chip, M_ROW, col]
                new_max = jnp.maximum(old_max, jnp.max(s, axis=0, keepdims=True))
                e = jnp.exp2(s * EXP_C - new_max * EXP_C)
                alphas[i] = jnp.exp2((old_max - new_max) * EXP_C)
                ACC[chip, M_ROW, col] = new_max
                ACC[chip, L_ROW, col] = ACC[chip, L_ROW, col] * alphas[i] + jnp.sum(e, axis=0, keepdims=True)
                probs[i] = e.astype(jnp.bfloat16)
            if i > 0:
                col = cols[i - 1]
                ACC[chip, O_ROWS, col] = ACC[chip, O_ROWS, col] * alphas[i - 1] + jnp.dot(
                    val_t, probs[i - 1], preferred_element_type=jnp.float32)

    def o_copy(dx):
        dst_x = (x + dx) % 4
        return remote(ACC.at[dst_x], PART.at[dx - 1], o_send.at[dx - 1], o_recv.at[dx - 1], dev(t, g * 4 + dst_x))

    def near(i, carry):
        h = lax.div(i, 2)
        a = 2 * lax.rem(i, 2) - 1
        for kind in range(3):
            def go():
                piece(kind, h, (a, 0), (a, 0), (a, 0)).wait_recv()

                @pl.when(a == -way(kind, h, True, a))
                def _():
                    piece(kind, h, (a, 0), (-a, 0), (2, 0)).start()

                spread(kind, h, a)
            when_live(kind, h, (a, 0), go)
        return carry

    lax.fori_loop(0, 4, near, 0)

    def far(h, carry):
        for kind in range(3):
            def go():
                piece(kind, h, (2, 0), (1, 0), (2, 0)).wait_recv()
                spread(kind, h, 2)
            when_live(kind, h, (2, 0), go)
        return carry

    def lines(i, carry):
        @pl.when(i == 4)
        def _():
            lax.fori_loop(0, 2, far, 0)
        a = offset(lax.div(i, 4))
        h = lax.rem(lax.div(i, 2), 2)
        b = 2 * lax.rem(i, 2) - 1
        for kind in range(3):
            def go():
                piece(kind, h, (a, b), (0, b), (a, b)).wait_recv()

                @pl.when(b == -way(kind, h, False, b))
                def _():
                    piece(kind, h, (a, b), (0, -b), (a, 2)).start()
            when_live(kind, h, (a, b), go)
        return carry

    lax.fori_loop(0, 16, lines, 0)

    def far_lines(i, carry):
        a = offset(lax.div(i, 2))
        h = lax.rem(i, 2)
        for kind in range(3):
            def go():
                piece(kind, h, (a, 2), (0, 1), (a, 2)).wait_recv()
            when_live(kind, h, (a, 2), go)
        return carry

    lax.fori_loop(0, 8, far_lines, 0)

    groups = plain_nb // 4
    for part in (0, 1):
        span = slice(part * GROUP // 2, (part + 1) * GROUP // 2)
        KC[nb // 4, span, :] = KVN[:, :, 0, part].reshape(GROUP // 2, HEAD_DIM)
        VC[nb // 4, :, span] = KVN[:, :, 1, part].reshape(GROUP // 2, HEAD_DIM).T
    for dx in (1, 3, 2):
        q_copy(dx, (x + 4 - dx) % 4).wait_recv()

    def chip_phase(phase, carry):
        for order, dx in ((1, 2), (2, 1), (3, 3)):
            @pl.when(phase == order)
            def _():
                o_copy(dx).start()
        dx = jnp.where(phase == 0, 2, jnp.where(phase == 1, 1, jnp.where(phase == 2, 3, 0)))
        chip = (x + dx) % 4

        def plain(n, inner):
            units(n, chip, False)
            return inner
        lax.fori_loop(0, groups, plain, 0)

        def masked(n, inner):
            units(groups + n, chip, True)
            return inner
        lax.fori_loop(0, cache_masked + 1, masked, 0)
        return carry

    lax.fori_loop(0, 4, chip_phase, 0)

    for dx in (1, 2, 3):
        q_copy(dx, x).wait_send()

    @pl.when(g < nb)
    def _():
        for cp in sib_copies(t):
            cp.wait_send()

    def drain(i, carry):
        h = lax.rem(i, 2)
        a, b = offset(lax.div(i, 8)), offset(lax.rem(lax.div(i, 2), 4))
        for kind in range(3):
            up = [-forward(kind, h)] * 2
            if kind < 2 and nb == 8:
                around = 2 * lax.rem(z, 2) - 1
                up = [jnp.where(h == 1, around, up[0]), jnp.where(h == 0, around, up[1])]
            first = jnp.where(b == 0, jnp.where(a == 2, up[0], 0), a)
            second = jnp.where(b == 2, up[1], 0)

            def go():
                piece(kind, h, (first, second), (1, 0), (a, b)).wait_send()

            def sent():
                when_live(kind, h, (first, second), go)
            pl.when(i >= 2)(sent)
        return carry

    lax.fori_loop(0, 32, drain, 0)

    for dx in (1, 3, 2):
        o_copy(dx).wait()
    maxes = [ACC[x, M_ROW, :]] + [PART[i, M_ROW, :] for i in range(3)]
    sums = [ACC[x, L_ROW, :]] + [PART[i, L_ROW, :] for i in range(3)]
    top = functools.reduce(jnp.maximum, maxes)
    weights = [jnp.exp2((m - top) * EXP_C) for m in maxes]
    total = sum(w * l for w, l in zip(weights, sums))
    acc = ACC[x, O_ROWS, :] * weights[0]
    for i in range(3):
        acc = acc + PART[i, O_ROWS, :] * weights[i + 1]
    o_rows = (acc / total).T.astype(jnp.bfloat16)
    heads = []
    for head in range(HEADS):
        pieces = []
        for core in (0, 1):
            for half in (0, 1):
                base = half * (COLS // 2) + head * 64 + core * 32
                pieces.append(o_rows[base:base + 32, :])
        heads.append(jnp.concatenate(pieces, axis=0))

    def add_over_cores(i):
        copy = remote(SUM.at[their_rows], GOT.at[i], x_send.at[2 + i], x_recv.at[2 + i], dev(1 - t, c))
        copy.start()
        copy.wait()
        return SUM[my_rows, :] + GOT[i]

    load_out.wait()
    share_norm(0).wait_send()
    NORM[0, :, 0:HEADS * HEAD_DIM] = jnp.concatenate(heads, axis=1)

    def project_out(i, carry):
        cols = pl.ds(pl.multiple_of(i * 512, 512), 512)
        SUM[:, cols] = jnp.dot(NORM[0, :, 0:HEADS * HEAD_DIM], WO[:, cols], preferred_element_type=jnp.float32)
        return carry

    lax.fori_loop(0, SUM.shape[1] // 512, project_out, 0)
    mid = (hid_ref[...].astype(jnp.float32) + add_over_cores(0)).astype(jnp.bfloat16).astype(jnp.float32)
    normed(1, mid)
    share_norm(1).start()
    norm_landed(1).wait_recv()
    share_norm(1).wait_send()

    def widen(i, carry):
        for cp in load_in(i):
            cp.wait()
        gate = jnp.dot(NORM[1], WG[lax.rem(i, held)], preferred_element_type=jnp.float32)
        up = jnp.dot(NORM[1], WU[lax.rem(i, held)], preferred_element_type=jnp.float32)
        HM[i] = (gate * jax.nn.sigmoid(gate) * up).astype(jnp.bfloat16)

        @pl.when(i + held < tiles)
        def _():
            for cp in load_in(i + held):
                cp.start()
        return carry

    lax.fori_loop(0, tiles, widen, 0)
    SUM[...] = jnp.zeros_like(SUM)

    def narrow(i, carry):
        load_down(i).wait()
        SUM[...] += jnp.dot(HM[i], WD[lax.rem(i, WD.shape[0])], preferred_element_type=jnp.float32)

        @pl.when(i + WD.shape[0] < tiles)
        def _():
            load_down(i + WD.shape[0]).start()
        return carry

    lax.fori_loop(0, tiles, narrow, 0)
    out_ref[...] = (mid + add_over_cores(1)).astype(jnp.bfloat16)


def layer(index, cache_len, table, hidden, gains, cache_k, cache_v, w_query, w_key, w_value, w_out, w_gate, w_up, w_down):
    nb = BUCKETS[index]
    masked = nb - (BUCKETS[index - 1] if index else 0)
    bf16, f32 = jnp.bfloat16, jnp.float32
    width, ffn = w_gate.shape
    tiles = ffn // FFN_TILE
    vmem = pl.BlockSpec(memory_space=pltpu.VMEM)
    hbm = pl.BlockSpec(memory_space=pl.ANY)
    dma = pltpu.SemaphoreType.DMA
    return pl.pallas_call(
        functools.partial(layer_kernel, nb, nb - masked),
        out_shape=jax.ShapeDtypeStruct(hidden.shape, bf16),
        in_specs=[pl.BlockSpec(memory_space=pltpu.SMEM)] + [vmem] * 5 + [hbm] * 7,
        out_specs=vmem,
        scratch_shapes=[
            pltpu.VMEM((4, HEAD_DIM, COLS), bf16),
            pltpu.VMEM((nb // 4 + 1, GROUP, HEAD_DIM), bf16),
            pltpu.VMEM((nb // 4 + 1, HEAD_DIM, GROUP), bf16),
            pltpu.VMEM((16, 2, 2, 2, 32, HEAD_DIM), bf16),
            pltpu.VMEM((4, 136, COLS), f32),
            pltpu.VMEM((3, 136, COLS), f32),
            pltpu.VMEM((TILE, SLOTS), bf16),
            pltpu.VMEM((masked // 4 + 1, GROUP, HEAD_DIM), jnp.int32),
            pltpu.VMEM(w_out.shape, bf16),
            pltpu.VMEM((HELD, width, FFN_TILE), bf16),
            pltpu.VMEM((HELD, width, FFN_TILE), bf16),
            pltpu.VMEM((HELD + 1, FFN_TILE, width), bf16),
            pltpu.VMEM((2, HEAD_DIM, width), bf16),
            pltpu.VMEM((HEAD_DIM, width), f32),
            pltpu.VMEM((2, 64, width), f32),
            pltpu.VMEM((tiles, HEAD_DIM, FFN_TILE), bf16),
            dma((2, 3, 16)), dma((2, 3, 16)), dma((3,)), dma((3,)), dma((3,)), dma((3,)), dma((2,)), dma((2,)), dma((2,)),
            dma((4, max(tiles, 4))), dma((4,)), dma((4,)),
        ],
        compiler_params=pltpu.CompilerParams(collective_id=index, has_side_effects=True, vmem_limit_bytes=67043328),
        name='layer_%d' % nb,
    )(cache_len, table, hidden, gains, cache_k, cache_v, w_query, w_key, w_value, w_out, w_gate, w_up, w_down)


def solution(mesh):
    token_spec = P(('dp', 'cp', 'tp'), None)
    column_spec = P(None, 'tp')
    row_spec = P('tp', None)

    def device_layer(hidden_loc, pos_loc, cache_len, cache_k, cache_v, norm1_gain, w_query, w_key, w_value, w_out, norm2_gain, w_gate, w_up, w_down):
        row = jnp.arange(HEAD_DIM, dtype=jnp.int32)
        run = 2 * lax.axis_index('cp') + row // 64
        run = jnp.where(row % 64 < 32, run, 255 - run)
        table = rotary_table(cache_len[0] + run * 32 + row % 32)
        gains = jnp.stack([norm1_gain, norm2_gain])
        bucket = sum((cache_len[0] > n * (8 * SLOTS)).astype(jnp.int32) for n in BUCKETS[:-1])
        return lax.switch(bucket, [functools.partial(layer, i) for i in range(len(BUCKETS))], cache_len, table, hidden_loc, gains,
                          cache_k, cache_v, w_query, w_key, w_value, w_out, w_gate, w_up, w_down)

    return jax.shard_map(device_layer, mesh=mesh, in_specs=(token_spec, P(('dp', 'cp', 'tp')), P('dp'), token_spec, token_spec, P(), column_spec, column_spec, column_spec, row_spec, P(), column_spec, column_spec, row_spec), out_specs=token_spec, check_vma=False)
```

```python
import functools
import math
import jax
import jax.numpy as jnp
from jax import lax
from jax.experimental import pallas as pl
from jax.experimental.pallas import tpu as pltpu
from jax.sharding import PartitionSpec as P

HEAD_DIM = 128
ROPE_BASE = 500000.0
NORM_EPS = 1e-5
HEADS = 6
SLOTS = 256
COLS = HEADS * 128
GROUP = 8 * SLOTS
FFN_TILE = 896
CACHE, NEW = (0, 1), (2,)
SIGNS = (1, -1)
AROUND = (1, 3, 2)
O_ROWS, M_ROW, L_ROW = slice(0, HEAD_DIM), slice(HEAD_DIM, HEAD_DIM + 1), slice(HEAD_DIM + 1, HEAD_DIM + 2)
TILE = 256
HELD = 3
NEG = -2.3e38
EXP_C = math.log2(math.e) / math.sqrt(HEAD_DIM)
BUCKETS = (8, 12, 16)


def rotary_table(positions):
    half_dim = HEAD_DIM // 2
    inv_freq = 1.0 / (ROPE_BASE ** (jnp.arange(half_dim, dtype=jnp.float32) * (2.0 / HEAD_DIM)))
    angles = positions.astype(jnp.float32)[:, None] * inv_freq[None, :]
    cos_table, sin_table = jnp.cos(angles), jnp.sin(angles)
    return jnp.stack([jnp.concatenate([cos_table, cos_table], axis=1), jnp.concatenate([-sin_table, sin_table], axis=1)])


def layer_kernel(nb, plain_nb, len_ref, table_ref, hid_ref, gain_ref, ck_ref, cv_ref,
                 wq_hbm, wk_hbm, wv_hbm, wo_hbm, wg_hbm, wu_hbm, wd_hbm, out_ref,
                 QT, KC, VC, KVN, ACC, PART, VTS, KPOS, WO, WG, WU, WD, NORM, SUM, GOT, HM,
                 send_sem, recv_sem, q_send, q_recv, o_send, o_recv, sib_send, sib_recv, loc_sem, w_sem, x_send, x_recv):
    c = lax.axis_index('cp')
    t = lax.axis_index('tp')
    x = c % 4
    g = c // 4
    cache_len = len_ref[0]
    cache_masked = (nb - plain_nb) // 4

    def dev(core, chip):
        return {'tp': core, 'cp': chip}

    z, y = g // 4, g % 4

    def place_at(h, a, b):
        c1 = lax.rem(y * (1 - h) + z * h + a + 4, 4)
        c2 = lax.rem(z * (1 - h) + y * h + b + 4, 4)
        return (4 * c2 + c1) * (1 - h) + (4 * c1 + c2) * h

    def offset(i):
        return jnp.where(i == 3, 2, jnp.where(i == 0, 0, 2 * i - 3))

    barrier = pltpu.get_barrier_semaphore()
    partners = [dev(t, place_at(0, a, b) * 4 + x) for a, b in ((-1, 0), (1, 0), (0, -1), (0, 1))]
    partners += [dev(t, g * 4 + (x + dx) % 4) for dx in AROUND] + [dev(1 - t, c)]
    for p in partners:
        pl.semaphore_signal(barrier, inc=1, device_id=p, device_id_type=pl.DeviceIdType.MESH)

    tiles = HM.shape[0]
    held = WG.shape[0]

    def load_in(i):
        cols = pl.ds(pl.multiple_of(i * FFN_TILE, HEAD_DIM), FFN_TILE)
        return (pltpu.make_async_copy(wg_hbm.at[:, cols], WG.at[lax.rem(i, held)], w_sem.at[1, i]),
                pltpu.make_async_copy(wu_hbm.at[:, cols], WU.at[lax.rem(i, held)], w_sem.at[2, i]))

    def load_down(i):
        return pltpu.make_async_copy(wd_hbm.at[pl.ds(i * FFN_TILE, FFN_TILE), :], WD.at[lax.rem(i, WD.shape[0])], w_sem.at[3, i])

    WQ = WG.at[held - 1, :, 0:HEADS * HEAD_DIM]
    WK, WV = WU.at[held - 1, :, 0:HEAD_DIM], WU.at[held - 1, :, HEAD_DIM:TILE]
    load_qkv = [pltpu.make_async_copy(wk_hbm, WK, w_sem.at[0, 0]), pltpu.make_async_copy(wv_hbm, WV, w_sem.at[0, 1]),
                pltpu.make_async_copy(wq_hbm, WQ, w_sem.at[0, 2])]
    load_out = pltpu.make_async_copy(wo_hbm, WO, w_sem.at[0, 3])
    for cp in load_qkv:
        cp.start()
    load_out.start()
    for i in range(held - 1):
        for cp in load_in(i):
            cp.start()
    for i in range(WD.shape[0]):
        load_down(i).start()

    my_rows = pl.ds(pl.multiple_of(t * 64, 64), 64)
    their_rows = pl.ds(pl.multiple_of((1 - t) * 64, 64), 64)

    def normed(i, values):
        inv_rms = lax.rsqrt(jnp.mean(values * values, axis=-1, keepdims=True) + NORM_EPS)
        NORM[i, my_rows, :] = (values * inv_rms * gain_ref[i:i + 1, :].astype(jnp.float32)).astype(jnp.bfloat16)

    VTS[...] = cv_ref[...].T
    normed(0, hid_ref[...].astype(jnp.float32))
    ACC[:, HEAD_DIM:136, :] = jnp.where(lax.broadcasted_iota(jnp.int32, (4, 8, COLS), 1) == 0, NEG, 0.0)
    ACC[:, O_ROWS, :] = jnp.zeros((4, HEAD_DIM, COLS), jnp.float32)
    row = lax.broadcasted_iota(jnp.int32, (GROUP, HEAD_DIM), 0)
    for i in range(cache_masked):
        slot_id = (4 * (plain_nb + 4 * i + row // (2 * SLOTS)) + x) * (2 * SLOTS) + row % (2 * SLOTS)
        KPOS[i] = jnp.where(slot_id < cache_len, -1, 1 << 30)
    run = 2 * (4 * (row % (GROUP // 2) // 64) + x) + (row % 64) // 32
    KPOS[cache_masked] = jnp.where(row < GROUP // 2, run, 255 - run) * 32 + row % 32
    pl.semaphore_wait(barrier, len(partners))

    def remote(src, dst, send, recv, device):
        return pltpu.make_async_remote_copy(src_ref=src, dst_ref=dst, send_sem=send, recv_sem=recv,
                                            device_id=device, device_id_type=pl.DeviceIdType.MESH)

    def q_copy(dx, chip_x):
        return remote(QT.at[x], QT.at[chip_x], q_send.at[dx - 1], q_recv.at[dx - 1], dev(t, g * 4 + (x + dx) % 4))

    def slot_of(kind, place, h):
        if kind == 2:
            return KVN.at[place, h]
        span = pl.ds(pl.multiple_of((lax.rem(place, 4) * 2 + h) * SLOTS, SLOTS), SLOTS)
        return KC.at[lax.div(place, 4), span, :] if kind == 0 else VC.at[lax.div(place, 4), :, span]

    mine = pl.ds(pl.multiple_of(t * HEAD_DIM, HEAD_DIM), HEAD_DIM)
    other = pl.ds(pl.multiple_of((1 - t) * HEAD_DIM, HEAD_DIM), HEAD_DIM)

    def sib_copies(h):
        return (remote(ck_ref.at[:, other], slot_of(0, g, h), sib_send.at[0], sib_recv.at[0], dev(1 - t, c)),
                remote(VTS.at[other], slot_of(1, g, h), sib_send.at[1], sib_recv.at[1], dev(1 - t, c)))

    local_cache = [pltpu.make_async_copy(ck_ref.at[:, mine], slot_of(0, g, t), loc_sem.at[0]),
                   pltpu.make_async_copy(VTS.at[mine], slot_of(1, g, t), loc_sem.at[1])]

    def share_norm(i):
        rows = NORM.at[i, my_rows]
        return remote(rows, rows, x_send.at[i], x_recv.at[i], dev(1 - t, c))

    def norm_landed(i):
        rows = NORM.at[i, their_rows]
        return remote(rows, rows, x_send.at[i], x_recv.at[i], dev(1 - t, c))

    share_norm(0).start()

    @pl.when(g < nb)
    def _():
        for cp in sib_copies(t):
            cp.start()
        for cp in local_cache:
            cp.start()

    def piece(kind, h, block, target, seen):
        place = place_at(h, *block)
        index = lax.rem(seen[0] + 4, 4) * 4 + lax.rem(seen[1] + 4, 4)
        ref = slot_of(kind, place, h)
        return remote(ref, ref, send_sem.at[h, kind, index], recv_sem.at[h, kind, index], dev(t, place_at(h, *target) * 4 + x))

    def when_live(kind, h, block, fn):
        if kind < 2:
            pl.when(place_at(h, *block) < nb)(fn)
        else:
            fn()

    def forward(kind, h):
        return (1, -1, 1 - 2 * h)[kind]

    def way(kind, h, first_axis, step):
        usual = forward(kind, h)
        if kind == 2 or nb != 8:
            return usual
        on_z = h if first_axis else 1 - h
        return jnp.where(on_z == 1, jnp.where(lax.rem(z + step + 4, 4) == 0, -1, 1), usual)

    def spread(kind, h, a):
        for sign in SIGNS:
            piece(kind, h, (a, 0), (0, sign), (a, -sign)).start()

    def own_sends(kinds):
        def body(h, carry):
            for kind in kinds:
                def go():
                    for sign in SIGNS:
                        piece(kind, h, (0, 0), (sign, 0), (-sign, 0)).start()
                    spread(kind, h, 0)
                when_live(kind, h, (0, 0), go)
            return carry
        lax.fori_loop(0, 2, body, 0)

    @pl.when(g < nb)
    def _():
        for cp in local_cache:
            cp.wait()
        for cp in sib_copies(1 - t):
            cp.wait_recv()

    own_sends(CACHE)

    norm_landed(0).wait_recv()

    def project(weight):
        return jnp.dot(NORM[0], weight, preferred_element_type=jnp.float32)

    def rotated(head):
        return (head * table_ref[0] + pltpu.roll(head, 64, 1) * table_ref[1]).astype(jnp.bfloat16)

    for cp in load_qkv[:2]:
        cp.wait()
    new_kv = (rotated(project(WK[...])), project(WV[...]).astype(jnp.bfloat16))
    for kv in (0, 1):
        for core in (0, 1):
            for half in (0, 1):
                base = core * 64 + half * 32
                KVN[g, core, kv, half] = new_kv[kv][base:base + 32, :]
    load_qkv[2].wait()

    def project_pair(i, carry):
        both = project(WG[held - 1, :, pl.ds(pl.multiple_of(i * TILE, TILE), TILE)])
        pair = [rotated(both[:, :HEAD_DIM]), rotated(both[:, HEAD_DIM:])]
        for half in (0, 1):
            rows = [head[core * 64 + half * 32:core * 64 + half * 32 + 32, :] for head in pair for core in (0, 1)]
            QT[x, :, pl.ds(pl.multiple_of(half * (COLS // 2) + i * HEAD_DIM, HEAD_DIM), HEAD_DIM)] = jnp.concatenate(rows, axis=0).T
        return carry

    lax.fori_loop(0, HEADS // 2, project_pair, 0)
    own_sends(NEW)
    for dx in (2, 1, 3):
        q_copy(dx, x).start()
    for cp in load_in(held - 1):
        cp.start()

    def units(group, chip, masked):
        cols = [pl.ds(tile * TILE, TILE) for tile in range(3)]
        key, val_t = KC[group], VC[group]

        def score(i):
            s = jnp.dot(key, QT[chip, :, cols[i]], preferred_element_type=jnp.float32)
            if masked:
                col = lax.broadcasted_iota(jnp.int32, (1, TILE), 1) + i * TILE
                late = col // (COLS // 2)
                q_run = 2 * (4 * g + chip) + (col % 64) // 32
                q_pos = (q_run + late * (255 - 2 * q_run)) * 32 + col % 32
                k_pos = KPOS[group - plain_nb // 4]
                seen = [k_pos <= q_pos[:, :HEAD_DIM], k_pos <= q_pos[:, HEAD_DIM:]]
                s = jnp.concatenate([jnp.where(seen[j], s[:, j * HEAD_DIM:j * HEAD_DIM + HEAD_DIM], NEG) for j in (0, 1)], axis=1)
            return s

        scores = [score(0)] + [None] * 2
        probs = [None] * 3
        alphas = [None] * 3
        for i in range(4):
            if i < 2:
                scores[i + 1] = score(i + 1)
            if i < 3:
                col, s = cols[i], scores[i]
                old_max = ACC[chip, M_ROW, col]
                new_max = jnp.maximum(old_max, jnp.max(s, axis=0, keepdims=True))
                e = jnp.exp2(s * EXP_C - new_max * EXP_C)
                alphas[i] = jnp.exp2((old_max - new_max) * EXP_C)
                ACC[chip, M_ROW, col] = new_max
                ACC[chip, L_ROW, col] = ACC[chip, L_ROW, col] * alphas[i] + jnp.sum(e, axis=0, keepdims=True)
                probs[i] = e.astype(jnp.bfloat16)
            if i > 0:
                col = cols[i - 1]
                ACC[chip, O_ROWS, col] = ACC[chip, O_ROWS, col] * alphas[i - 1] + jnp.dot(
                    val_t, probs[i - 1], preferred_element_type=jnp.float32)

    def o_copy(dx):
        dst_x = (x + dx) % 4
        return remote(ACC.at[dst_x], PART.at[dx - 1], o_send.at[dx - 1], o_recv.at[dx - 1], dev(t, g * 4 + dst_x))

    def near(kinds, i, carry):
        h = lax.div(i, 2)
        a = 2 * lax.rem(i, 2) - 1
        for kind in kinds:
            def go():
                piece(kind, h, (a, 0), (a, 0), (a, 0)).wait_recv()

                @pl.when(a == -way(kind, h, True, a))
                def _():
                    piece(kind, h, (a, 0), (-a, 0), (2, 0)).start()

                spread(kind, h, a)
            when_live(kind, h, (a, 0), go)
        return carry

    def far(h, carry):
        for kind in CACHE + NEW:
            def go():
                piece(kind, h, (2, 0), (1, 0), (2, 0)).wait_recv()
                spread(kind, h, 2)
            when_live(kind, h, (2, 0), go)
        return carry

    def lines(kinds, i, carry):
        a = offset(lax.div(i, 4))
        h = lax.rem(lax.div(i, 2), 2)
        b = 2 * lax.rem(i, 2) - 1
        for kind in kinds:
            def go():
                piece(kind, h, (a, b), (0, b), (a, b)).wait_recv()

                @pl.when(b == -way(kind, h, False, b))
                def _():
                    piece(kind, h, (a, b), (0, -b), (a, 2)).start()
            when_live(kind, h, (a, b), go)
        return carry

    for kinds in (CACHE, NEW):
        lax.fori_loop(0, 4, functools.partial(near, kinds), 0)
        lax.fori_loop(0, 4, functools.partial(lines, kinds), 0)
    lax.fori_loop(0, 2, far, 0)
    lax.fori_loop(4, 16, functools.partial(lines, CACHE + NEW), 0)

    def far_lines(i, carry):
        a = offset(lax.div(i, 2))
        h = lax.rem(i, 2)
        for kind in CACHE + NEW:
            def go():
                piece(kind, h, (a, 2), (0, 1), (a, 2)).wait_recv()
            when_live(kind, h, (a, 2), go)
        return carry

    lax.fori_loop(0, 8, far_lines, 0)

    groups = plain_nb // 4
    for part in (0, 1):
        span = slice(part * GROUP // 2, (part + 1) * GROUP // 2)
        KC[nb // 4, span, :] = KVN[:, :, 0, part].reshape(GROUP // 2, HEAD_DIM)
        VC[nb // 4, :, span] = KVN[:, :, 1, part].reshape(GROUP // 2, HEAD_DIM).T
    for dx in AROUND:
        q_copy(dx, (x + 4 - dx) % 4).wait_recv()

    def chip_phase(phase, carry):
        for order, dx in ((1, 2), (2, 1), (3, 3)):
            @pl.when(phase == order)
            def _():
                o_copy(dx).start()
        dx = jnp.where(phase == 0, 2, jnp.where(phase == 1, 1, jnp.where(phase == 2, 3, 0)))
        chip = (x + dx) % 4

        def plain(n, inner):
            units(n, chip, False)
            return inner
        lax.fori_loop(0, groups, plain, 0)

        def masked(n, inner):
            units(groups + n, chip, True)
            return inner
        lax.fori_loop(0, cache_masked + 1, masked, 0)
        return carry

    lax.fori_loop(0, 4, chip_phase, 0)

    for dx in AROUND:
        q_copy(dx, x).wait_send()

    @pl.when(g < nb)
    def _():
        for cp in sib_copies(t):
            cp.wait_send()

    def drain(i, carry):
        h = lax.rem(i, 2)
        a, b = offset(lax.div(i, 8)), offset(lax.rem(lax.div(i, 2), 4))
        for kind in CACHE + NEW:
            up = [-forward(kind, h)] * 2
            if kind < 2 and nb == 8:
                around = 2 * lax.rem(z, 2) - 1
                up = [jnp.where(h == 1, around, up[0]), jnp.where(h == 0, around, up[1])]
            first = jnp.where(b == 0, jnp.where(a == 2, up[0], 0), a)
            second = jnp.where(b == 2, up[1], 0)

            def go():
                piece(kind, h, (first, second), (1, 0), (a, b)).wait_send()

            def sent():
                when_live(kind, h, (first, second), go)
            pl.when(i >= 2)(sent)
        return carry

    lax.fori_loop(0, 32, drain, 0)

    for dx in AROUND:
        o_copy(dx).wait()
    maxes = [ACC[x, M_ROW, :]] + [PART[i, M_ROW, :] for i in range(3)]
    sums = [ACC[x, L_ROW, :]] + [PART[i, L_ROW, :] for i in range(3)]
    top = functools.reduce(jnp.maximum, maxes)
    weights = [jnp.exp2((m - top) * EXP_C) for m in maxes]
    total = sum(w * l for w, l in zip(weights, sums))
    acc = ACC[x, O_ROWS, :] * weights[0]
    for i in range(3):
        acc = acc + PART[i, O_ROWS, :] * weights[i + 1]
    o_rows = (acc / total).T.astype(jnp.bfloat16)
    heads = []
    for head in range(HEADS):
        pieces = []
        for core in (0, 1):
            for half in (0, 1):
                base = half * (COLS // 2) + head * 64 + core * 32
                pieces.append(o_rows[base:base + 32, :])
        heads.append(jnp.concatenate(pieces, axis=0))

    def add_over_cores(i):
        copy = remote(SUM.at[their_rows], GOT.at[i], x_send.at[2 + i], x_recv.at[2 + i], dev(1 - t, c))
        copy.start()
        copy.wait()
        return SUM[my_rows, :] + GOT[i]

    load_out.wait()
    share_norm(0).wait_send()
    NORM[0, :, 0:HEADS * HEAD_DIM] = jnp.concatenate(heads, axis=1)

    def project_out(i, carry):
        cols = pl.ds(pl.multiple_of(i * 512, 512), 512)
        SUM[:, cols] = jnp.dot(NORM[0, :, 0:HEADS * HEAD_DIM], WO[:, cols], preferred_element_type=jnp.float32)
        return carry

    lax.fori_loop(0, SUM.shape[1] // 512, project_out, 0)
    mid = (hid_ref[...].astype(jnp.float32) + add_over_cores(0)).astype(jnp.bfloat16).astype(jnp.float32)
    normed(1, mid)
    share_norm(1).start()
    norm_landed(1).wait_recv()
    share_norm(1).wait_send()

    def widen(i, carry):
        for cp in load_in(i):
            cp.wait()
        gate = jnp.dot(NORM[1], WG[lax.rem(i, held)], preferred_element_type=jnp.float32)
        up = jnp.dot(NORM[1], WU[lax.rem(i, held)], preferred_element_type=jnp.float32)
        HM[i] = (gate * jax.nn.sigmoid(gate) * up).astype(jnp.bfloat16)

        @pl.when(i + held < tiles)
        def _():
            for cp in load_in(i + held):
                cp.start()
        return carry

    lax.fori_loop(0, tiles, widen, 0)
    SUM[...] = jnp.zeros_like(SUM)

    def narrow(i, carry):
        load_down(i).wait()
        SUM[...] += jnp.dot(HM[i], WD[lax.rem(i, WD.shape[0])], preferred_element_type=jnp.float32)

        @pl.when(i + WD.shape[0] < tiles)
        def _():
            load_down(i + WD.shape[0]).start()
        return carry

    lax.fori_loop(0, tiles, narrow, 0)
    out_ref[...] = (mid + add_over_cores(1)).astype(jnp.bfloat16)


def layer(index, cache_len, table, hidden, gains, cache_k, cache_v, w_query, w_key, w_value, w_out, w_gate, w_up, w_down):
    nb = BUCKETS[index]
    masked = nb - (BUCKETS[index - 1] if index else 0)
    bf16, f32 = jnp.bfloat16, jnp.float32
    width, ffn = w_gate.shape
    tiles = ffn // FFN_TILE
    vmem = pl.BlockSpec(memory_space=pltpu.VMEM)
    hbm = pl.BlockSpec(memory_space=pl.ANY)
    dma = pltpu.SemaphoreType.DMA
    return pl.pallas_call(
        functools.partial(layer_kernel, nb, nb - masked),
        out_shape=jax.ShapeDtypeStruct(hidden.shape, bf16),
        in_specs=[pl.BlockSpec(memory_space=pltpu.SMEM)] + [vmem] * 5 + [hbm] * 7,
        out_specs=vmem,
        scratch_shapes=[
            pltpu.VMEM((4, HEAD_DIM, COLS), bf16),
            pltpu.VMEM((nb // 4 + 1, GROUP, HEAD_DIM), bf16),
            pltpu.VMEM((nb // 4 + 1, HEAD_DIM, GROUP), bf16),
            pltpu.VMEM((16, 2, 2, 2, 32, HEAD_DIM), bf16),
            pltpu.VMEM((4, 136, COLS), f32),
            pltpu.VMEM((3, 136, COLS), f32),
            pltpu.VMEM((TILE, SLOTS), bf16),
            pltpu.VMEM((masked // 4 + 1, GROUP, HEAD_DIM), jnp.int32),
            pltpu.VMEM(w_out.shape, bf16),
            pltpu.VMEM((HELD, width, FFN_TILE), bf16),
            pltpu.VMEM((HELD, width, FFN_TILE), bf16),
            pltpu.VMEM((HELD + 1, FFN_TILE, width), bf16),
            pltpu.VMEM((2, HEAD_DIM, width), bf16),
            pltpu.VMEM((HEAD_DIM, width), f32),
            pltpu.VMEM((2, 64, width), f32),
            pltpu.VMEM((tiles, HEAD_DIM, FFN_TILE), bf16),
            dma((2, 3, 16)), dma((2, 3, 16)), dma((3,)), dma((3,)), dma((3,)), dma((3,)), dma((2,)), dma((2,)), dma((2,)),
            dma((4, max(tiles, 4))), dma((4,)), dma((4,)),
        ],
        compiler_params=pltpu.CompilerParams(collective_id=index, has_side_effects=True, vmem_limit_bytes=67043328),
        name='layer_%d' % nb,
    )(cache_len, table, hidden, gains, cache_k, cache_v, w_query, w_key, w_value, w_out, w_gate, w_up, w_down)


def solution(mesh):
    token_spec = P(('dp', 'cp', 'tp'), None)
    column_spec = P(None, 'tp')
    row_spec = P('tp', None)

    def device_layer(hidden_loc, pos_loc, cache_len, cache_k, cache_v, norm1_gain, w_query, w_key, w_value, w_out, norm2_gain, w_gate, w_up, w_down):
        row = jnp.arange(HEAD_DIM, dtype=jnp.int32)
        run = 2 * lax.axis_index('cp') + row // 64
        run = jnp.where(row % 64 < 32, run, 255 - run)
        table = rotary_table(cache_len[0] + run * 32 + row % 32)
        gains = jnp.stack([norm1_gain, norm2_gain])
        bucket = sum((cache_len[0] > n * (8 * SLOTS)).astype(jnp.int32) for n in BUCKETS[:-1])
        return lax.switch(bucket, [functools.partial(layer, i) for i in range(len(BUCKETS))], cache_len, table, hidden_loc, gains,
                          cache_k, cache_v, w_query, w_key, w_value, w_out, w_gate, w_up, w_down)

    return jax.shard_map(device_layer, mesh=mesh, in_specs=(token_spec, P(('dp', 'cp', 'tp')), P('dp'), token_spec, token_spec, P(), column_spec, column_spec, column_spec, row_spec, P(), column_spec, column_spec, row_spec), out_specs=token_spec, check_vma=False)
```
